256 devices in a mesh: tm: 8 (over x_lo, y), lat: 16 (over z, x_hi), ens: 2 (over core).
Axes of the slice: x: 4 (x_hi: 2, x_lo: 2; x = x_hi * 2 + x_lo), y: 4, z: 8, core: 2. Of those that a mesh axis runs over, the one named last changes fastest.
Arguments:
- increment: float32 [8, 8, 256, 1440], P('tm', None, 'lat'), may hold values from -6 to 6
- wind_lon: float32 [8, 8, 256, 1440], P('tm', None, 'lat'), may hold values from -0.45 to 0.45
- wind_lat: float32 [8, 8, 256, 1440], P('tm', None, 'lat'), may hold values from -0.45 to 0.45
- model_precision: float32 [8], replicated, may hold values from 0.5 to 4
- perturbations: float32 [32, 8, 256, 1440], P('ens', 'tm', 'lat'), may hold values from -0.14478652 to 0.14478652
- obs_rows: int32 [8, 512], P('tm', 'lat'), may hold values from 0 to 127
- obs_jacobian: float32 [8, 512, 16, 1440], P('tm', 'lat'), may hold values from -0.15625 to 0.15625
- obs_values: float32 [8, 512, 16], P('tm', 'lat'), may hold values from -6 to 6
- obs_precision: float32 [8, 512, 16], P('tm', 'lat'), may hold values from 0.5 to 2
- obs_counts: int32 [8, 512], P('tm', 'lat'), may hold values from 1 to 16
Outputs:
- grad_state: float32 [8, 8, 256, 1440], P('tm', None, 'lat')
- forcing_step: float32 [8, 256, 1440], P('tm', 'lat')
The draws below stay inside these ranges and needn't reach their ends.
Inputs may be any that keep to these rules, and one draw needn't show every extreme that they name: `obs_rows`: block j of band b reads level r // 16 and latitude b * 16 + r % 16, where r is its entry; several blocks may read the same row. `obs_counts`: only the first count slots of a block hold observations.
All inputs are finite; a program needn't handle non-finite values.
Results may differ from the reference program's by a relative error of at most 0.0003.
Values sent between devices are 32-bit elements; how exact they have to be, the bound alone decides.
No kernel may reach another device: no remote copies, remote signals or barrier semaphores. Data moves between devices by JAX's collectives and lax.ppermute only.
A program may use at most 64 MiB of HBM per device.

```python
import math
import jax
import jax.numpy as jnp
from jax import lax

NLON = 1440
MEM = 32
CLAT = 16
STEPS = 4
OBS = 32
NOB = 16
NT = 8
LEV = 8
NLAT = 256
OBSALL = 512


def with_ends(entries, rng, least, top_value):
    longest = entries.shape.index(max(entries.shape))
    spots = []
    for shift in (0, 1):
        where = [jax.random.randint(jax.random.fold_in(rng, axis), (), 0, length) for axis, length in enumerate(entries.shape)]
        where[longest] = (where[longest] + shift) % entries.shape[longest]
        spots.append(tuple(where))
    return entries.at[spots[0]].set(least).at[spots[1]].set(top_value)


def shard_levels(own_key, extent, split, least, top_value):
    level = 1.0
    for axis_at, shards_of in split:
        draws = jax.random.uniform(jax.random.fold_in(jax.random.fold_in(own_key, 6), axis_at), (shards_of,), jnp.float32, least / len(split), top_value / len(split))
        level = level * jnp.repeat(jnp.exp(draws), extent[axis_at] // shards_of).reshape((-1,) + (1,) * (len(extent) - 1 - axis_at))
    return level


def noise(rng, extent, spread, most, pieces=(), kind=jnp.bfloat16):
    loudness = shard_levels(rng, extent, pieces, -0.22, 0.18) if pieces else 1.0
    entries = jax.random.normal(rng, extent, jnp.float32) * spread * loudness
    return jnp.minimum(jnp.maximum(entries, -most), most).astype(kind)


def setup_inputs(seed: int = 0) -> dict:
    arg_keys = jax.random.split(jax.random.key(seed), 11)
    return {
        "increment": noise(arg_keys[0], (NT, LEV, NLAT, NLON), 1.0, 6.0, ((0, 8), (2, 16)), jnp.float32),
        "wind_lon": jnp.clip(jax.random.uniform(arg_keys[1], (NT, LEV, NLAT, NLON), jnp.float32, -0.45, 0.45) * shard_levels(arg_keys[1], (NT, LEV, NLAT, NLON), ((0, 8), (2, 16)), -0.4, 0.0), -0.45, 0.45),
        "wind_lat": jnp.clip(jax.random.uniform(arg_keys[2], (NT, LEV, NLAT, NLON), jnp.float32, -0.45, 0.45) * shard_levels(arg_keys[2], (NT, LEV, NLAT, NLON), ((0, 8), (2, 16)), -0.4, 0.0), -0.45, 0.45),
        "model_precision": jnp.clip(jnp.exp(jax.random.uniform(arg_keys[3], (LEV,), jnp.float32, math.log(0.5), math.log(4.0))), 0.5, 4.0),
        "perturbations": noise(arg_keys[4], (MEM, LEV, NLAT, NLON), ((LEV * NLAT * NLON) ** -0.25), 0.14478652, ((0, 2), (1, 8), (2, 16)), jnp.float32),
        "obs_rows": with_ends(jax.random.randint(arg_keys[5], (NT, OBSALL), 0, LEV * CLAT), jax.random.fold_in(arg_keys[5], 1), 0, (LEV * CLAT) - 1).astype(jnp.int32),
        "obs_jacobian": noise(arg_keys[6], (NT, OBSALL, NOB, NLON), NLON ** -0.5, 0.15625, ((0, 8), (1, 16)), jnp.float32),
        "obs_values": noise(arg_keys[7], (NT, OBSALL, NOB), 1.0, 6.0, ((0, 8), (1, 16)), jnp.float32),
        "obs_precision": jnp.clip(jnp.exp(math.log(2.0) - 1.3862944 * jax.random.uniform(arg_keys[8], (NT, OBSALL, NOB), jnp.float32) ** shard_levels(arg_keys[8], (NT, OBSALL, NOB), ((0, 8), (1, 16)), -0.2, 0.2)), 0.5, 2.0),
        "obs_counts": with_ends(jax.random.randint(arg_keys[9], (NT, OBSALL), 1, NOB + 1), jax.random.fold_in(arg_keys[9], 1), 1, NOB).astype(jnp.int32),
    }


def coefficients(wind_lon, wind_lat):
    center = 1.0 - wind_lon * wind_lon - wind_lat * wind_lat
    plus_lon = 0.5 * (wind_lon * wind_lon - wind_lon)
    minus_lon = 0.5 * (wind_lon * wind_lon + wind_lon)
    plus_lat = 0.5 * (wind_lat * wind_lat - wind_lat)
    minus_lat = 0.5 * (wind_lat * wind_lat + wind_lat)
    return (center, plus_lon, minus_lon, plus_lat, minus_lat)


def advect(field, coefs):
    center, plus_lon, minus_lon, plus_lat, minus_lat = coefs
    northern = jnp.pad(field[:, 1:], ((0, 0), (0, 1), (0, 0)))
    southern = jnp.pad(field[:, :-1], ((0, 0), (1, 0), (0, 0)))
    return (center * field + plus_lon * jnp.roll(field, -1, 2) + minus_lon * jnp.roll(field, 1, 2)
            + plus_lat * northern + minus_lat * southern)


def advect_adjoint(field, coefs):
    center, plus_lon, minus_lon, plus_lat, minus_lat = coefs
    upward = plus_lat * field
    downward = minus_lat * field
    from_south = jnp.pad(upward[:, :-1], ((0, 0), (1, 0), (0, 0)))
    from_north = jnp.pad(downward[:, 1:], ((0, 0), (0, 1), (0, 0)))
    return (center * field + jnp.roll(plus_lon * field, 1, 2) + jnp.roll(minus_lon * field, -1, 2)
            + from_south + from_north)


def reference(increment, wind_lon, wind_lat, model_precision, perturbations, obs_rows, obs_jacobian,
              obs_values, obs_precision, obs_counts):
    highest = lax.Precision.HIGHEST
    level_prec = model_precision[:, None, None]
    band = jnp.arange(OBSALL, dtype=jnp.int32) // OBS
    slots = jnp.arange(NOB, dtype=jnp.int32)
    ends = []
    coef_list = []
    for window in range(NT):
        coefs = coefficients(wind_lon[window], wind_lat[window])
        coef_list.append(coefs)
        field = increment[window]
        for repeat in range(STEPS):
            field = advect(field, coefs)
        ends.append(field)
    mismatches = []
    for window in range(NT):
        if window > 0:
            mismatches.append(level_prec * (increment[window] - ends[window - 1]))
        else:
            mismatches.append(level_prec * increment[window])
    grads = []
    total = jnp.zeros((LEV, NLAT, NLON), jnp.float32)
    for window in range(NT):
        coefs = coef_list[window]
        rows = obs_rows[window].astype(jnp.int32)
        level = rows // CLAT
        latitude = band * CLAT + rows % CLAT
        picked = ends[window][level, latitude]
        jacobian = obs_jacobian[window]
        evolved = jnp.einsum('jon,jn->jo', jacobian, picked, precision=highest)
        used = (slots[None, :] < obs_counts[window][:, None]).astype(jnp.float32)
        weighted = obs_precision[window] * (evolved - obs_values[window]) * used
        force = jnp.einsum('jon,jo->jn', jacobian, weighted, precision=highest)
        adjoint = jnp.zeros((LEV, NLAT, NLON), jnp.float32).at[level, latitude].add(force)
        if window + 1 < NT:
            adjoint = adjoint - mismatches[window + 1]
        forcing = adjoint
        for repeat in range(STEPS):
            adjoint = advect_adjoint(adjoint, coefs)
            if repeat + 1 < STEPS:
                forcing = forcing + adjoint
        grads.append(adjoint + mismatches[window])
        total = total + forcing
    member_coef = jnp.einsum('mlan,lan->m', perturbations, total, precision=highest)
    forcing_step = -jnp.einsum('m,mlan->lan', member_coef, perturbations, precision=highest) / (MEM - 1.0)
    return jnp.stack(grads), forcing_step
```

```python
import jax
import jax.numpy as jnp
from jax import lax
from jax.experimental import pallas as pl
from jax.experimental.pallas import tpu as pltpu
from jax.sharding import Mesh
from jax.sharding import PartitionSpec as P

MEM = 32
STEPS = 4
LANES = 128
TM = ("tm_0", "tm_1")
LAT = ("lat_0", "lat_1")
ALL = ("tm_0", "tm_1", "lat_0", "lat_1", "ens")


def wrapped(value):
    lon = value.shape[-1]
    half = (-lon % LANES) // 2
    return jnp.concatenate([value, value[..., :half], value[..., lon - half :]], axis=-1)


def row_major(value):
    return wrapped(jnp.swapaxes(value, 0, 1))


def east(value):
    return pltpu.roll(value, value.shape[-1] - 1, 1)


def west(value):
    return pltpu.roll(value, 1, 1)


def forward_kernel(
    core_ref, rows_ref, prec_ref, inc_ref, lon_ref, lat_ref, halo_ref, next_ref, jac_ref, val_ref, oprec_ref,
    used_ref, end_ref, adj_ref, outer_ref, inner_ref, coef_ref, x0, x1, pk, wgt,
):
    core = core_ref[0]
    has_next = core_ref[1]
    blocks, slots, lons = jac_ref.shape
    own_at = 4 * (1 - core)
    x0[pl.ds(own_at, 12)] = inc_ref[...]
    x0[pl.ds(12 * core, 4)] = halo_ref[0:4]
    center, plon, mlon, plat, mlat = (coef_ref.at[i] for i in range(5))

    def fill(at, c, e):
        cc = c * c
        ee = e * e
        center[at] = 1.0 - cc - ee
        plon[at] = 0.5 * (cc - c)
        mlon[at] = 0.5 * (cc + c)
        plat[at] = 0.5 * (ee - e)
        mlat[at] = 0.5 * (ee + e)

    for r in range(12):
        fill(own_at + r, lon_ref[r], lat_ref[r])
    for r in range(3):
        fill(1 + 11 * core + r, halo_ref[4 + r], halo_ref[7 + r])
    ones = jnp.ones(x0.shape[1:], jnp.float32)

    @pl.when(core == 0)
    def _():
        plat[0] = ones

    @pl.when(core == 1)
    def _():
        mlat[15] = ones

    bufs = (x0, x1)
    for step in range(STEPS):
        src, dst = bufs[step % 2], bufs[(step + 1) % 2]
        for j in range(step + 1, 15 - step):
            f = src[j]
            dst[j] = (
                center[j] * f + plon[j] * east(f) + mlon[j] * west(f) + plat[j] * src[j + 1] + mlat[j] * src[j - 1]
            )
    field = bufs[STEPS % 2]
    prec = prec_ref[...] * has_next.astype(jnp.float32)
    for r in range(8):
        f = field[4 + r]
        end_ref[r] = f
        adj_ref[r] = prec * (f - next_ref[r])

    lane = lax.broadcasted_iota(jnp.int32, (slots, LANES), 1)
    for j in range(blocks):
        r = rows_ref[0, j]
        row = jnp.clip(r % 16 - 8 * core, 0, 7)
        pk[pl.ds(j, 1), :] = field[4 + row, pl.ds(r // 16, 1), :]
    ev = jnp.zeros((slots, LANES), jnp.float32)
    for j in range(blocks):
        total = jnp.sum(jac_ref[j] * pk[pl.ds(j, 1), 0:lons], axis=1, keepdims=True)
        ev = jnp.where(lane == j, total, ev)
    wgt[...] = oprec_ref[...] * (ev - val_ref[...]) * used_ref[...]
    for j in range(blocks):
        w = jnp.sum(jnp.where(lane == j, wgt[...], 0.0), axis=1, keepdims=True)
        force = jnp.sum(jac_ref[j] * w, axis=0, keepdims=True)
        pk[pl.ds(j, 1), 0:lons] = force
    lane32 = lax.broadcasted_iota(jnp.int32, (blocks, LANES), 1)
    tail = lons % LANES
    first = pk[:, 0:LANES]
    last = pk[:, lons - tail :]
    half = (LANES - tail) // 2
    pk[:, lons - tail :] = jnp.where(
        lane32 < tail, last, jnp.where(lane32 < tail + half, pltpu.roll(first, tail, 1), pltpu.roll(last, LANES - tail, 1))
    )
    for j in range(blocks):
        r = rows_ref[0, j]
        row = jnp.clip(r % 16 - 8 * core, 0, 7)
        lev = pl.ds(r // 16, 1)
        adj_ref[row, lev, :] = adj_ref[row, lev, :] + pk[pl.ds(j, 1), :]

    @pl.when(core == 0)
    def _():
        for r in range(4):
            outer_ref[r] = adj_ref[r] * mlat[7] if r == 3 else adj_ref[r]
            inner_ref[r] = adj_ref[4 + r]

    @pl.when(core == 1)
    def _():
        for r in range(4):
            outer_ref[r] = adj_ref[4 + r] * plat[8] if r == 0 else adj_ref[4 + r]
            inner_ref[r] = adj_ref[r]


def adjoint_kernel(core_ref, adj_ref, outer_ref, inner_ref, coef_ref, forcing_ref, start_ref, g0, g1):
    core = core_ref[0]
    lons = forcing_ref.shape[-1]
    center, plon, mlon, plat, mlat = (coef_ref.at[i] for i in range(5))
    g0[4:12] = adj_ref[...]
    g0[pl.ds(12 * core, 4)] = outer_ref[...]
    g0[pl.ds(12 * (1 - core), 4)] = inner_ref[...]
    bufs = (g0, g1)
    acc = [None] * 8
    for step in range(STEPS):
        src, dst = bufs[step % 2], bufs[(step + 1) % 2]
        for j in range(step + 1, 15 - step):
            g = src[j]
            out = (
                center[j] * g
                + west(plon[j] * g)
                + east(mlon[j] * g)
                + plat[j - 1] * src[j - 1]
                + mlat[j + 1] * src[j + 1]
            )
            if step + 1 < STEPS:
                dst[j] = out
            else:
                start_ref[j - 4] = out
            if 4 <= j < 12 and step + 1 < STEPS:
                acc[j - 4] = (src[j] if step == 0 else acc[j - 4]) + out
    for r in range(8):
        forcing_ref[:, r, :] = acc[r][:, 0:lons]


def product_kernel(core_ref, pieces_ref, own_ref, other_ref, out_ref):
    core = core_ref[0]
    forcing = jnp.sum(pieces_ref[...], axis=0)
    first = pl.multiple_of(8 * core, 8)
    lane = lax.broadcasted_iota(jnp.int32, (8, LANES), 1)
    members = own_ref.shape[0]
    vec = jnp.zeros((8, LANES), jnp.float32)
    for m in range(2 * members):
        ref, at = (own_ref, m) if m < members else (other_ref, m - members)
        col = jnp.sum(ref[at, 0, pl.ds(first, 8), :] * forcing, axis=1, keepdims=True)
        vec = jnp.where(lane == m, col, vec)
    vec = jnp.sum(vec, axis=0, keepdims=True)
    swapped = jnp.where(
        lane[0:1] < members, pltpu.roll(vec, LANES - members, 1), pltpu.roll(vec, members, 1)
    )
    vec = jnp.where(core == 0, vec, swapped)
    vec = jnp.where(lane[0:1] < 2 * members, vec, 0.0)
    out_ref[...] = jnp.broadcast_to(vec[None], out_ref.shape)


def step_kernel(core_ref, sums_ref, own_ref, other_ref, out_ref):
    core = core_ref[0]
    members = own_ref.shape[0]
    vec = jnp.sum(sums_ref[...], axis=0)
    swapped = jnp.where(
        lax.broadcasted_iota(jnp.int32, (1, LANES), 1) < members,
        pltpu.roll(vec, LANES - members, 1),
        pltpu.roll(vec, members, 1),
    )
    vec = jnp.where(core == 0, vec, swapped) * (-1.0 / (MEM - 1.0))
    wide = jnp.broadcast_to(vec, (8, LANES))
    lane = lax.broadcasted_iota(jnp.int32, (8, LANES), 1)
    coefs = [jnp.sum(jnp.where(lane == m, wide, 0.0), axis=1, keepdims=True) for m in range(2 * members)]
    for half in range(2):
        rows = pl.ds(8 * half, 8)
        total = coefs[0] * own_ref[0, 0, rows, :]
        for m in range(1, 2 * members):
            ref, at = (own_ref, m) if m < members else (other_ref, m - members)
            total = total + coefs[m] * ref[at, 0, rows, :]
        out_ref[0, rows, :] = total


VMEM = pl.BlockSpec(memory_space=pltpu.VMEM)
SMEM = pl.BlockSpec(memory_space=pltpu.SMEM)


def call(kernel, ins, outs, scratch=(), limit=40):
    return pl.pallas_call(
        kernel,
        out_shape=[jax.ShapeDtypeStruct(s, jnp.float32) for s in outs],
        in_specs=ins,
        out_specs=[VMEM] * len(outs),
        scratch_shapes=[pltpu.VMEM(s, jnp.float32) for s in scratch],
        compiler_params=pltpu.CompilerParams(vmem_limit_bytes=limit * 2**20),
        name=kernel.__name__,
    )


def on_device(
    increment,
    wind_lon,
    wind_lat,
    model_precision,
    perturbations,
    obs_rows,
    obs_jacobian,
    obs_values,
    obs_precision,
    obs_counts,
):
    core = lax.axis_index("ens")
    count_t = lax.axis_size(TM)
    count_l = lax.axis_size(LAT)
    has_next = (lax.axis_index(TM) < count_t - 1).astype(jnp.int32)
    flags = jnp.stack([core, has_next]).astype(jnp.int32)
    levels, band_rows, lons = increment.shape[1:]
    wide = lons + (-lons % LANES)

    def rows_of(value, start, size):
        return lax.dynamic_slice_in_dim(value[0], start, size, axis=1)

    trade = []
    for i in range(count_l - 1):
        trade += [(2 * i + 1, 2 * i + 2), (2 * i + 2, 2 * i + 1)]
    partner = [(0, 1), (1, 0)]
    outgoing = row_major(
        jnp.concatenate(
            [rows_of(increment, 12 * core, 4), rows_of(wind_lon, 13 * core, 3), rows_of(wind_lat, 13 * core, 3)], axis=1
        )
    )
    halo = lax.ppermute(outgoing, LAT + ("ens",), trade)
    own_rows = row_major(rows_of(increment, 8 * core, 8))
    next_rows = lax.ppermute(own_rows, TM, [(i + 1, i) for i in range(count_t - 1)])
    other_pert = lax.ppermute(perturbations, "ens", partner)

    inc12 = row_major(rows_of(increment, 4 * core, 12))
    lon12 = row_major(rows_of(wind_lon, 4 * core, 12))
    lat12 = row_major(rows_of(wind_lat, 4 * core, 12))
    prec = jnp.broadcast_to(model_precision[:, None], (levels, wide))
    blocks, slots = obs_values.shape[1:]

    def by_slot(value):
        return jnp.pad(value.T, ((0, 0), (0, LANES - blocks)))

    slot = jnp.arange(slots, dtype=jnp.int32)
    mine = (obs_rows[0] % band_rows) // 8 == core
    used = ((slot[None, :] < obs_counts[0][:, None]) & mine[:, None]).astype(jnp.float32)

    own_shape = (8, levels, wide)
    end, adj, outer, inner, coefs = call(
        forward_kernel,
        [SMEM, SMEM] + [VMEM] * 10,
        [own_shape, own_shape, (4, levels, wide), (4, levels, wide), (5, 16, levels, wide)],
        [(16, levels, wide), (16, levels, wide), (blocks, wide), (slots, LANES)],
    )(
        flags, obs_rows, prec, inc12, lon12, lat12, halo, next_rows, obs_jacobian[0],
        by_slot(obs_values[0]), by_slot(obs_precision[0]), by_slot(used),
    )
    outer = lax.ppermute(outer, LAT + ("ens",), trade)
    inner = lax.ppermute(inner, "ens", partner)
    prior = lax.ppermute(end, TM, [(i, i + 1) for i in range(count_t - 1)])

    forcing, start = call(
        adjoint_kernel,
        [SMEM] + [VMEM] * 4,
        [(levels, 8, lons), own_shape],
        [(16, levels, wide), (16, levels, wide)],
    )(flags, adj, outer, inner, coefs)
    pieces = lax.all_to_all(forcing, TM, 0, 0, tiled=True)

    own_grad = start[..., :lons] + model_precision[:, None] * (own_rows[..., :lons] - prior[..., :lons])
    other_grad = lax.ppermute(own_grad, "ens", partner)
    grad = jnp.where(
        core == 0,
        jnp.concatenate([own_grad, other_grad], axis=0),
        jnp.concatenate([other_grad, own_grad], axis=0),
    )
    grad_state = jnp.swapaxes(grad, 0, 1)[None]

    peers = lax.axis_size(ALL)
    (products,) = call(product_kernel, [SMEM] + [VMEM] * 3, [(peers, 1, LANES)])(
        flags, pieces, perturbations, other_pert
    )
    sums = lax.all_to_all(products, ALL, 0, 0, tiled=True)
    (forcing_step,) = call(step_kernel, [SMEM] + [VMEM] * 3, [(1, band_rows, lons)])(
        flags, sums, perturbations, other_pert
    )
    return (grad_state, forcing_step)


def solution(mesh):
    torus = Mesh(
        mesh.devices.reshape(2, 4, 8, 2, mesh.shape["ens"]),
        ("tm_0", "tm_1", "lat_0", "lat_1", "ens"),
    )
    in_specs = (
        P(TM, None, LAT, None),
        P(TM, None, LAT, None),
        P(TM, None, LAT, None),
        P(),
        P("ens", TM, LAT, None),
        P(TM, LAT),
        P(TM, LAT, None, None),
        P(TM, LAT, None),
        P(TM, LAT, None),
        P(TM, LAT),
    )
    out_specs = (P(TM, None, LAT, None), P(TM, LAT, None))
    return jax.shard_map(
        on_device, mesh=torus, in_specs=in_specs, out_specs=out_specs, check_vma=False
    )
```

```python
import jax
import jax.numpy as jnp
from jax import lax
from jax.experimental import pallas as pl
from jax.experimental.pallas import tpu as pltpu
from jax.sharding import Mesh
from jax.sharding import PartitionSpec as P

MEM = 32
STEPS = 4
LANES = 128
HALF = 8
TM = ("tm_0", "tm_1")
LAT = ("lat_0", "lat_1")
TM_LAT = ("tm_0", "tm_1", "lat_0", "lat_1")


def east(value):
    return pltpu.roll(value, value.shape[-1] - 1, 1)


def west(value):
    return pltpu.roll(value, 1, 1)


def wrap(ref, lons):
    tail = lons % LANES
    half = (LANES - tail) // 2
    first = ref[:, 0:LANES]
    lane = lax.broadcasted_iota(jnp.int32, first.shape, 1)
    last = jnp.where(lane < tail, ref[:, lons - tail :], 0.0)
    ref[:, lons - tail :] = jnp.where(
        lane < tail, last, jnp.where(lane < tail + half, pltpu.roll(first, tail, 1), pltpu.roll(last, LANES - tail, 1))
    )


def fetch(source, first, size, target, sem):
    return pltpu.make_async_copy(source.at[0, :, pl.ds(first, size), :], target, sem)


def edge_kernel(inc_hbm, lon_hbm, lat_hbm, out_ref, inc, lon, lat, sems):
    core = lax.axis_index("ens")
    lons = inc.shape[-1]
    levels = inc.shape[0]

    def rows(first, at):
        copies = [
            fetch(source, first, HALF, target, sems.at[i])
            for i, (source, target) in enumerate(((inc_hbm, inc), (lon_hbm, lon), (lat_hbm, lat)))
        ]
        for copy in copies:
            copy.start()
        sign = 1.0 if at(0) == 7 else -1.0
        for i, copy in enumerate(copies):
            copy.wait()
            buf = (inc, lon, lat)[i]
            base = (0, 4, 7)[i]
            for q in range(4 if i == 0 else 3):
                r = 3 - q if i == 0 else 2 - q
                value = buf[:, at(r), :]
                if i == 2:
                    value = sign * value
                out_ref[base + q, :, 0:lons] = value
                wrap(out_ref.at[base + q], lons)

    @pl.when(core == 0)
    def _():
        rows(0, lambda r: r)

    @pl.when(core == 1)
    def _():
        rows(HALF, lambda r: 7 - r)


def prepare_kernel(inc_hbm, lon_hbm, lat_hbm, prec_ref, own_ref, field_ref, coef_ref, prec_out, inc, lon, lat, sems):
    core = lax.axis_index("ens")
    lons = inc.shape[-1]
    levels = inc.shape[0]
    copies = [
        fetch(source, 0, 2 * HALF, target, sems.at[i])
        for i, (source, target) in enumerate(((inc_hbm, inc), (lon_hbm, lon), (lat_hbm, lat)))
    ]
    for copy in copies:
        copy.start()
    level = lax.broadcasted_iota(jnp.int32, prec_out.shape, 0)
    prec = jnp.zeros(prec_out.shape, jnp.float32)
    for k in range(levels):
        prec = jnp.where(level == k, prec_ref[k], prec)
    prec_out[...] = prec
    for copy in copies:
        copy.wait()

    def rows(at, sign):
        for r in range(12):
            field_ref[r, :, 0:lons] = inc[:, at(r), :]
            wrap(field_ref.at[r], lons)
            if r < HALF:
                own_ref[r] = field_ref[r]
            coef_ref[1, r, :, 0:lons] = lon[:, at(r), :]
            wrap(coef_ref.at[1, r], lons)
            coef_ref[4, r, :, 0:lons] = sign * lat[:, at(r), :]
            wrap(coef_ref.at[4, r], lons)
            store_coefficients(coef_ref, r, coef_ref[1, r], coef_ref[4, r])

    @pl.when(core == 0)
    def _():
        rows(lambda r: r, 1.0)

    @pl.when(core == 1)
    def _():
        rows(lambda r: 15 - r, -1.0)


def store_coefficients(coef_ref, at, c, e):
    cc = c * c
    ee = e * e
    coef_ref[0, at] = 1.0 - cc - ee
    coef_ref[1, at] = 0.5 * (cc - c)
    coef_ref[2, at] = 0.5 * (cc + c)
    coef_ref[3, at] = 0.5 * (ee - e)
    coef_ref[4, at] = 0.5 * (ee + e)


class Rows:
    def __init__(self, halo_ref, own_ref, at):
        self.halo, self.own, self.at = halo_ref, own_ref, at

    def __getitem__(self, j):
        return self.halo[self.at, j] if j < 4 else self.own[self.at, j - 4]


def forward_kernel(
    field_ref, coef_ref, prec_ref, halo_ref, next_ref, jac_hbm, rows_hbm, rows_ref, counts_ref, val_ref, oprec_ref,
    later_ref, adj_ref, outer_ref, inner_ref, edge_ref, x0, x1, pk, wgt, jac, rows, sems,
):
    core = lax.axis_index("ens")
    has_next = (lax.axis_index(TM) < lax.axis_size(TM) - 1).astype(jnp.float32)
    blocks, slots, lons = jac.shape
    jac_copy = pltpu.make_async_copy(jac_hbm.at[0], jac, sems.at[0])
    rows_copy = pltpu.make_async_copy(rows_hbm, rows, sems.at[1])
    jac_copy.start()
    rows_copy.start()
    x0[0:4] = halo_ref[0:4]
    x0[4:16] = field_ref[...]
    center, plon, mlon, plat, mlat = (Rows(edge_ref, coef_ref, i) for i in range(5))
    edge_ref[3, 0] = jnp.ones(x0.shape[1:], jnp.float32)
    for r in range(3):
        store_coefficients(edge_ref, 1 + r, halo_ref[4 + r], halo_ref[7 + r])

    bufs = (x0, x1)
    for step in range(STEPS):
        src, dst = bufs[step % 2], bufs[(step + 1) % 2]
        for j in range(step + 1, 15 - step):
            f = src[j]
            dst[j] = (
                center[j] * f + plon[j] * east(f) + mlon[j] * west(f) + plat[j] * src[j + 1] + mlat[j] * src[j - 1]
            )
    field = bufs[STEPS % 2]
    prec = prec_ref[...] * has_next
    for r in range(HALF):
        later = prec * (next_ref[r] - field[4 + r])
        later_ref[r] = later
        adj_ref[r] = -later

    rows_copy.wait()
    jac_copy.wait()

    def place(j):
        r = rows[0, j]
        lat = r % 16
        row = jnp.clip(jnp.where(core == 0, lat, 15 - lat), 0, HALF - 1)
        return row, pl.ds(r // 16, 1)

    for j in range(blocks):
        row, lev = place(j)
        pk[pl.ds(j, 1), :] = field[4 + row, lev, :]
    lane = lax.broadcasted_iota(jnp.int32, (slots, blocks), 1)
    slot = lax.broadcasted_iota(jnp.int32, (slots, blocks), 0)
    ev = jnp.zeros((slots, blocks), jnp.float32)
    for j in range(blocks):
        total = jnp.sum(jac[j] * pk[pl.ds(j, 1), 0:lons], axis=1, keepdims=True)
        ev = jnp.where(lane == j, total, ev)
    mine = (rows_ref[...] % 16) // HALF == core
    used = (slot < counts_ref[...]) & mine
    wgt[...] = jnp.where(used, oprec_ref[...] * (ev - val_ref[...]), 0.0)
    for j in range(blocks):
        w = jnp.sum(jnp.where(lane == j, wgt[...], 0.0), axis=1, keepdims=True)
        pk[pl.ds(j, 1), 0:lons] = jnp.sum(jac[j] * w, axis=0, keepdims=True)
    wrap(pk, lons)
    for j in range(blocks):
        row, lev = place(j)
        adj_ref[row, lev, :] = adj_ref[row, lev, :] + pk[pl.ds(j, 1), :]

    for q in range(4):
        outer_ref[q] = adj_ref[3 - q] * mlat[7] if q == 0 else adj_ref[3 - q]
        inner_ref[q] = adj_ref[7 - q]


def adjoint_kernel(adj_ref, outer_ref, inner_ref, edge_ref, coef_ref, forcing_ref, start_ref, g0, g1, total):
    core = lax.axis_index("ens")
    lons = forcing_ref.shape[-1]
    center, plon, mlon, plat, mlat = (Rows(edge_ref, coef_ref, i) for i in range(5))
    g0[0:4] = outer_ref[...]
    g0[4:12] = adj_ref[...]
    g0[12:16] = inner_ref[...]
    bufs = (g0, g1)
    for step in range(STEPS):
        src, dst = bufs[step % 2], bufs[(step + 1) % 2]
        for j in range(step + 1, 15 - step):
            g = src[j]
            out = (
                center[j] * g
                + west(plon[j] * g)
                + east(mlon[j] * g)
                + plat[j - 1] * src[j - 1]
                + mlat[j + 1] * src[j + 1]
            )
            if step + 1 < STEPS:
                dst[j] = out
                if 4 <= j < 12:
                    total[j - 4] = (g if step == 0 else total[j - 4]) + out
            else:
                start_ref[j - 4] = out

    @pl.when(core == 0)
    def _():
        for r in range(HALF):
            forcing_ref[:, r, :] = total[r, :, 0:lons]

    @pl.when(core == 1)
    def _():
        for r in range(HALF):
            forcing_ref[:, 7 - r, :] = total[r, :, 0:lons]


def product_kernel(pieces_ref, own_ref, other_ref, start_ref, mismatch_ref, inc_ref, prec_ref, out_ref, grad_ref):
    core = lax.axis_index("ens")
    first_window = lax.axis_index(TM) == 0
    prec = prec_ref[...]
    for r in range(HALF):
        grad_ref[r] = start_ref[r] + jnp.where(first_window, prec * inc_ref[r], mismatch_ref[r])
    forcing = jnp.sum(pieces_ref[...], axis=0)
    lane = lax.broadcasted_iota(jnp.int32, (HALF, LANES), 1)
    members = own_ref.shape[0]
    first = pl.multiple_of(HALF * core, HALF)
    vec = jnp.zeros((HALF, LANES), jnp.float32)
    for m in range(2 * members):
        ref, at = (own_ref, m) if m < members else (other_ref, m - members)
        col = jnp.sum(ref[at, 0, pl.ds(first, HALF), :] * forcing, axis=1, keepdims=True)
        vec = jnp.where(lane == m, col, vec)
    vec = jnp.sum(vec, axis=0, keepdims=True)
    out_ref[...] = jnp.broadcast_to(vec[None], out_ref.shape)


def sum_kernel(sums_ref, out_ref):
    vec = jnp.sum(sums_ref[...], axis=0)
    out_ref[...] = jnp.broadcast_to(vec, out_ref.shape)


def step_kernel(sum_ref, other_sum_ref, own_ref, other_ref, out_ref):
    members = own_ref.shape[0]
    lane = lax.broadcasted_iota(jnp.int32, (HALF, LANES), 1)
    theirs = other_sum_ref[...]
    swapped = jnp.where(
        lane < members, pltpu.roll(theirs, LANES - members, 1), pltpu.roll(theirs, members, 1)
    )
    vec = (sum_ref[...] + swapped) * (-1.0 / (MEM - 1.0))
    coefs = [jnp.sum(jnp.where(lane == m, vec, 0.0), axis=1, keepdims=True) for m in range(2 * members)]
    for half in range(2):
        rows = pl.ds(HALF * half, HALF)
        total = coefs[0] * own_ref[0, 0, rows, :]
        for m in range(1, 2 * members):
            ref, at = (own_ref, m) if m < members else (other_ref, m - members)
            total = total + coefs[m] * ref[at, 0, rows, :]
        out_ref[0, rows, :] = total


def gradient_kernel(own_ref, other_ref, out_ref):
    core = lax.axis_index("ens")
    lons = out_ref.shape[-1]

    def store(north, south):
        for r in range(HALF):
            out_ref[0, :, r, :] = north[r, :, 0:lons]
            out_ref[0, :, 15 - r, :] = south[r, :, 0:lons]

    @pl.when(core == 0)
    def _():
        store(own_ref, other_ref)

    @pl.when(core == 1)
    def _():
        store(other_ref, own_ref)


VMEM = pl.BlockSpec(memory_space=pltpu.VMEM)
SMEM = pl.BlockSpec(memory_space=pltpu.SMEM)
ANY = pl.BlockSpec(memory_space=pl.ANY)
HBM = pl.BlockSpec(memory_space=pltpu.HBM)


def buf(*shape):
    return pltpu.VMEM(shape, jnp.float32)


def call(kernel, ins, outs, scratch=(), limit=40):
    return pl.pallas_call(
        kernel,
        out_shape=[jax.ShapeDtypeStruct(s, jnp.float32) for s in outs],
        in_specs=ins,
        out_specs=[VMEM] * len(outs),
        scratch_shapes=list(scratch),
        compiler_params=pltpu.CompilerParams(vmem_limit_bytes=limit * 2**20),
    )


def on_device(
    increment,
    wind_lon,
    wind_lat,
    model_precision,
    perturbations,
    obs_rows,
    obs_jacobian,
    obs_values,
    obs_precision,
    obs_counts,
):
    count_t = lax.axis_size(TM)
    count_l = lax.axis_size(LAT)
    levels, band_rows, lons = increment.shape[1:]
    wide = lons + (-lons % LANES)
    blocks, slots = obs_values.shape[1:]

    trade = []
    for i in range(count_l - 1):
        trade += [(2 * i + 1, 2 * i + 2), (2 * i + 2, 2 * i + 1)]
    band = LAT + ("ens",)
    partner = [(0, 1), (1, 0)]
    own = (HALF, levels, wide)
    quarter = (4, levels, wide)
    fields = (increment, wind_lon, wind_lat)
    piece = buf(levels, HALF, lons)
    whole = buf(levels, band_rows, lons)

    (outgoing,) = call(
        edge_kernel, [HBM] * 3, [(10, levels, wide)], [piece, piece, piece, pltpu.SemaphoreType.DMA((3,))]
    )(*fields)
    halo = lax.ppermute(outgoing, band, trade)
    own_rows, field, coefs, prec = call(
        prepare_kernel,
        [ANY] * 3 + [SMEM],
        [own, (12, levels, wide), (5, 12, levels, wide), (levels, wide)],
        [whole, whole, whole, pltpu.SemaphoreType.DMA((3,))],
    )(*fields, model_precision)
    next_rows = lax.ppermute(own_rows, TM, [(i + 1, i) for i in range(count_t - 1)])
    other_pert = lax.ppermute(perturbations, "ens", partner)

    later, adj, outer, inner, edges = call(
        forward_kernel,
        [VMEM] * 5 + [ANY, ANY] + [VMEM] * 4,
        [own, own, quarter, quarter, (5, 4, levels, wide)],
        [
            buf(16, levels, wide), buf(16, levels, wide), buf(blocks, wide), buf(slots, blocks),
            buf(blocks, slots, lons), pltpu.SMEM((1, blocks), jnp.int32), pltpu.SemaphoreType.DMA((2,)),
        ],
    )(
        field, coefs, prec, halo, next_rows, obs_jacobian, obs_rows, obs_rows, obs_counts,
        obs_values[0].T, obs_precision[0].T,
    )
    outer = lax.ppermute(outer, band, trade)
    inner = lax.ppermute(inner, "ens", partner)
    mismatch = lax.ppermute(later, TM, [(i, i + 1) for i in range(count_t - 1)])

    forcing, start = call(
        adjoint_kernel,
        [VMEM] * 5,
        [(levels, HALF, lons), own],
        [buf(16, levels, wide), buf(16, levels, wide), buf(*own)],
    )(adj, outer, inner, edges, coefs)
    forcing, mismatch = lax.optimization_barrier((forcing, mismatch))
    pieces = lax.all_to_all(forcing, TM, 0, 0, tiled=True)

    products, own_grad = call(product_kernel, [VMEM] * 7, [(count_t * count_l, 1, LANES), own])(
        pieces, perturbations, other_pert, start, mismatch, own_rows, prec
    )
    other_grad = lax.ppermute(own_grad, "ens", partner)
    sums = lax.all_to_all(products, TM_LAT, 0, 0, tiled=True)
    (grad_state,) = call(gradient_kernel, [VMEM] * 2, [(1, levels, band_rows, lons)])(own_grad, other_grad)

    (total,) = call(sum_kernel, [VMEM], [(HALF, LANES)])(sums)
    other_total = lax.ppermute(total, "ens", partner)
    (forcing_step,) = call(step_kernel, [VMEM] * 4, [(1, band_rows, lons)])(
        total, other_total, perturbations, other_pert
    )
    return (grad_state, forcing_step)


def solution(mesh):
    torus = Mesh(
        mesh.devices.reshape(2, 4, 8, 2, mesh.shape["ens"]),
        ("tm_0", "tm_1", "lat_0", "lat_1", "ens"),
    )
    in_specs = (
        P(TM, None, LAT, None),
        P(TM, None, LAT, None),
        P(TM, None, LAT, None),
        P(),
        P("ens", TM, LAT, None),
        P(TM, LAT),
        P(TM, LAT, None, None),
        P(TM, LAT, None),
        P(TM, LAT, None),
        P(TM, LAT),
    )
    out_specs = (P(TM, None, LAT, None), P(TM, LAT, None))

    return jax.shard_map(on_device, mesh=torus, in_specs=in_specs, out_specs=out_specs, check_vma=False)
```

```python
import jax
import jax.numpy as jnp
from jax import lax
from jax.experimental import pallas as pl
from jax.experimental.pallas import tpu as pltpu
from jax.sharding import Mesh
from jax.sharding import PartitionSpec as P

MEM = 32
STEPS = 4
LANES = 128
HALF = 8
TM = ("tm_0", "tm_1")
LAT = ("lat_0", "lat_1")
TM_LAT = ("tm_0", "tm_1", "lat_0", "lat_1")


def east(value):
    return pltpu.roll(value, value.shape[-1] - 1, 1)


def west(value):
    return pltpu.roll(value, 1, 1)


def wrap(ref, lons):
    tail = lons % LANES
    half = (LANES - tail) // 2
    first = ref[:, 0:LANES]
    lane = lax.broadcasted_iota(jnp.int32, first.shape, 1)
    last = jnp.where(lane < tail, ref[:, lons - tail :], 0.0)
    ref[:, lons - tail :] = jnp.where(
        lane < tail, last, jnp.where(lane < tail + half, pltpu.roll(first, tail, 1), pltpu.roll(last, LANES - tail, 1))
    )


def fetch(source, first, size, target, sem):
    return pltpu.make_async_copy(source.at[0, :, pl.ds(first, size), :], target, sem)


def edge_kernel(inc_hbm, lon_hbm, lat_hbm, out_ref, inc, lon, lat, sems):
    core = lax.axis_index("ens")
    lons = inc.shape[-1]
    levels = inc.shape[0]

    def rows(first, at):
        copies = [
            fetch(source, first, HALF, target, sems.at[i])
            for i, (source, target) in enumerate(((inc_hbm, inc), (lon_hbm, lon), (lat_hbm, lat)))
        ]
        for copy in copies:
            copy.start()
        sign = 1.0 if at(0) == 7 else -1.0
        for i, copy in enumerate(copies):
            copy.wait()
            buf = (inc, lon, lat)[i]
            base = (0, 4, 7)[i]
            for q in range(4 if i == 0 else 3):
                r = 3 - q if i == 0 else 2 - q
                value = buf[:, at(r), :]
                if i == 2:
                    value = sign * value
                out_ref[base + q, :, 0:lons] = value
                wrap(out_ref.at[base + q], lons)

    @pl.when(core == 0)
    def _():
        rows(0, lambda r: r)

    @pl.when(core == 1)
    def _():
        rows(HALF, lambda r: 7 - r)


def own_kernel(inc_ref, own_ref, field_ref):
    core = lax.axis_index("ens")
    lons = inc_ref.shape[-1]

    def rows(at):
        for r in range(12):
            field_ref[r, :, 0:lons] = inc_ref[0, :, at(r), :]
            wrap(field_ref.at[r], lons)
            if r < HALF:
                own_ref[r] = field_ref[r]

    @pl.when(core == 0)
    def _():
        rows(lambda r: r)

    @pl.when(core == 1)
    def _():
        rows(lambda r: 15 - r)


def prepare_kernel(
    lon_hbm, lat_hbm, prec_ref, rows_ref, counts_ref, oprec_ref, coef_ref, prec_out, weight_ref, lon, lat, sems
):
    core = lax.axis_index("ens")
    lons = lon.shape[-1]
    levels = lon.shape[0]
    copies = [
        fetch(source, 0, 2 * HALF, target, sems.at[i])
        for i, (source, target) in enumerate(((lon_hbm, lon), (lat_hbm, lat)))
    ]
    for copy in copies:
        copy.start()
    level = lax.broadcasted_iota(jnp.int32, prec_out.shape, 0)
    prec = jnp.zeros(prec_out.shape, jnp.float32)
    for k in range(levels):
        prec = jnp.where(level == k, prec_ref[k], prec)
    prec_out[...] = prec
    slot = lax.broadcasted_iota(jnp.int32, weight_ref.shape, 0)
    mine = (rows_ref[...] % 16) // HALF == core
    weight_ref[...] = jnp.where((slot < counts_ref[...]) & mine, oprec_ref[...], 0.0)
    for copy in copies:
        copy.wait()

    def rows(at, sign):
        for r in range(12):
            coef_ref[1, r, :, 0:lons] = lon[:, at(r), :]
            wrap(coef_ref.at[1, r], lons)
            coef_ref[4, r, :, 0:lons] = sign * lat[:, at(r), :]
            wrap(coef_ref.at[4, r], lons)
            store_coefficients(coef_ref, r, coef_ref[1, r], coef_ref[4, r])

    @pl.when(core == 0)
    def _():
        rows(lambda r: r, 1.0)

    @pl.when(core == 1)
    def _():
        rows(lambda r: 15 - r, -1.0)


def store_coefficients(coef_ref, at, c, e):
    cc = c * c
    ee = e * e
    coef_ref[0, at] = 1.0 - cc - ee
    coef_ref[1, at] = 0.5 * (cc - c)
    coef_ref[2, at] = 0.5 * (cc + c)
    coef_ref[3, at] = 0.5 * (ee - e)
    coef_ref[4, at] = 0.5 * (ee + e)


class Rows:
    def __init__(self, halo_ref, own_ref, at):
        self.halo, self.own, self.at = halo_ref, own_ref, at

    def __getitem__(self, j):
        return self.halo[self.at, j] if j < 4 else self.own[self.at, j - 4]


def forward_kernel(
    field_ref, coef_ref, prec_ref, halo_ref, next_ref, jac_hbm, rows_hbm, val_ref, weight_ref,
    later_ref, adj_ref, outer_ref, inner_ref, edge_ref, x0, x1, pk, wgt, jac, rows, sems,
):
    core = lax.axis_index("ens")
    has_next = (lax.axis_index(TM) < lax.axis_size(TM) - 1).astype(jnp.float32)
    blocks, slots, lons = jac.shape
    jac_copy = pltpu.make_async_copy(jac_hbm.at[0], jac, sems.at[0])
    rows_copy = pltpu.make_async_copy(rows_hbm, rows, sems.at[1])
    jac_copy.start()
    rows_copy.start()
    x0[0:4] = halo_ref[0:4]
    x0[4:16] = field_ref[...]
    center, plon, mlon, plat, mlat = (Rows(edge_ref, coef_ref, i) for i in range(5))
    edge_ref[3, 0] = jnp.ones(x0.shape[1:], jnp.float32)
    for r in range(3):
        store_coefficients(edge_ref, 1 + r, halo_ref[4 + r], halo_ref[7 + r])

    bufs = (x0, x1)
    for step in range(STEPS):
        src, dst = bufs[step % 2], bufs[(step + 1) % 2]
        for j in range(step + 1, 15 - step):
            f = src[j]
            dst[j] = (
                center[j] * f + plon[j] * east(f) + mlon[j] * west(f) + plat[j] * src[j + 1] + mlat[j] * src[j - 1]
            )
    field = bufs[STEPS % 2]
    prec = prec_ref[...] * has_next
    for r in range(HALF):
        later = prec * (next_ref[r] - field[4 + r])
        later_ref[r] = later
        adj_ref[r] = -later

    rows_copy.wait()
    jac_copy.wait()

    def place(j):
        r = rows[0, j]
        lat = r % 16
        row = jnp.clip(jnp.where(core == 0, lat, 15 - lat), 0, HALF - 1)
        return row, pl.ds(r // 16, 1)

    for j in range(blocks):
        row, lev = place(j)
        pk[pl.ds(j, 1), :] = field[4 + row, lev, :]
    lane = lax.broadcasted_iota(jnp.int32, (slots, blocks), 1)
    ev = jnp.zeros((slots, blocks), jnp.float32)
    for j in range(blocks):
        total = jnp.sum(jac[j] * pk[pl.ds(j, 1), 0:lons], axis=1, keepdims=True)
        ev = jnp.where(lane == j, total, ev)
    wgt[...] = weight_ref[...] * (ev - val_ref[...])
    for j in range(blocks):
        w = jnp.sum(jnp.where(lane == j, wgt[...], 0.0), axis=1, keepdims=True)
        pk[pl.ds(j, 1), 0:lons] = jnp.sum(jac[j] * w, axis=0, keepdims=True)
    wrap(pk, lons)
    for j in range(blocks):
        row, lev = place(j)
        adj_ref[row, lev, :] = adj_ref[row, lev, :] + pk[pl.ds(j, 1), :]

    for q in range(4):
        outer_ref[q] = adj_ref[3 - q] * mlat[7] if q == 0 else adj_ref[3 - q]
        inner_ref[q] = adj_ref[7 - q]


def adjoint_kernel(adj_ref, outer_ref, inner_ref, edge_ref, coef_ref, forcing_ref, start_ref, g0, g1, total):
    core = lax.axis_index("ens")
    lons = forcing_ref.shape[-1]
    center, plon, mlon, plat, mlat = (Rows(edge_ref, coef_ref, i) for i in range(5))
    g0[0:4] = outer_ref[...]
    g0[4:12] = adj_ref[...]
    g0[12:16] = inner_ref[...]
    bufs = (g0, g1)
    for step in range(STEPS):
        src, dst = bufs[step % 2], bufs[(step + 1) % 2]
        for j in range(step + 1, 15 - step):
            g = src[j]
            out = (
                center[j] * g
                + west(plon[j] * g)
                + east(mlon[j] * g)
                + plat[j - 1] * src[j - 1]
                + mlat[j + 1] * src[j + 1]
            )
            if step + 1 < STEPS:
                dst[j] = out
                if 4 <= j < 12:
                    total[j - 4] = (g if step == 0 else total[j - 4]) + out
            else:
                start_ref[j - 4] = out

    @pl.when(core == 0)
    def _():
        for r in range(HALF):
            forcing_ref[:, r, :] = total[r, :, 0:lons]

    @pl.when(core == 1)
    def _():
        for r in range(HALF):
            forcing_ref[:, 7 - r, :] = total[r, :, 0:lons]


def mismatch_kernel(start_ref, mismatch_ref, inc_ref, prec_ref, grad_ref):
    first_window = lax.axis_index(TM) == 0
    prec = prec_ref[...]
    for r in range(HALF):
        grad_ref[r] = start_ref[r] + jnp.where(first_window, prec * inc_ref[r], mismatch_ref[r])


def product_kernel(pieces_ref, own_ref, other_ref, out_ref):
    core = lax.axis_index("ens")
    forcing = jnp.sum(pieces_ref[...], axis=0)
    lane = lax.broadcasted_iota(jnp.int32, (HALF, LANES), 1)
    members = own_ref.shape[0]
    first = pl.multiple_of(HALF * core, HALF)
    vec = jnp.zeros((HALF, LANES), jnp.float32)
    for m in range(2 * members):
        ref, at = (own_ref, m) if m < members else (other_ref, m - members)
        col = jnp.sum(ref[at, 0, pl.ds(first, HALF), :] * forcing, axis=1, keepdims=True)
        vec = jnp.where(lane == m, col, vec)
    vec = jnp.sum(vec, axis=0, keepdims=True)
    out_ref[...] = jnp.broadcast_to(vec[None], out_ref.shape)


def sum_kernel(sums_ref, out_ref):
    vec = jnp.sum(sums_ref[...], axis=0)
    out_ref[...] = jnp.broadcast_to(vec, out_ref.shape)


def step_kernel(sum_ref, other_sum_ref, own_ref, other_ref, out_ref):
    members = own_ref.shape[0]
    lane = lax.broadcasted_iota(jnp.int32, (HALF, LANES), 1)
    theirs = other_sum_ref[...]
    swapped = jnp.where(
        lane < members, pltpu.roll(theirs, LANES - members, 1), pltpu.roll(theirs, members, 1)
    )
    vec = (sum_ref[...] + swapped) * (-1.0 / (MEM - 1.0))
    coefs = [jnp.sum(jnp.where(lane == m, vec, 0.0), axis=1, keepdims=True) for m in range(2 * members)]
    for half in range(2):
        rows = pl.ds(HALF * half, HALF)
        total = coefs[0] * own_ref[0, 0, rows, :]
        for m in range(1, 2 * members):
            ref, at = (own_ref, m) if m < members else (other_ref, m - members)
            total = total + coefs[m] * ref[at, 0, rows, :]
        out_ref[0, rows, :] = total


def gradient_kernel(own_ref, other_ref, out_ref):
    core = lax.axis_index("ens")
    lons = out_ref.shape[-1]

    def store(north, south):
        for r in range(HALF):
            out_ref[0, :, r, :] = north[r, :, 0:lons]
            out_ref[0, :, 15 - r, :] = south[r, :, 0:lons]

    @pl.when(core == 0)
    def _():
        store(own_ref, other_ref)

    @pl.when(core == 1)
    def _():
        store(other_ref, own_ref)


VMEM = pl.BlockSpec(memory_space=pltpu.VMEM)
SMEM = pl.BlockSpec(memory_space=pltpu.SMEM)
HBM = pl.BlockSpec(memory_space=pltpu.HBM)


def buf(*shape):
    return pltpu.VMEM(shape, jnp.float32)


def in_hbm(value):
    return pltpu.with_memory_space_constraint(value, pltpu.HBM)


def call(kernel, ins, outs, scratch=(), limit=40):
    return pl.pallas_call(
        kernel,
        out_shape=[jax.ShapeDtypeStruct(s, jnp.float32) for s in outs],
        in_specs=ins,
        out_specs=[VMEM] * len(outs),
        scratch_shapes=list(scratch),
        compiler_params=pltpu.CompilerParams(vmem_limit_bytes=int(limit * 2**20)),
    )


def on_device(
    increment,
    wind_lon,
    wind_lat,
    model_precision,
    perturbations,
    obs_rows,
    obs_jacobian,
    obs_values,
    obs_precision,
    obs_counts,
):
    count_t = lax.axis_size(TM)
    count_l = lax.axis_size(LAT)
    levels, band_rows, lons = increment.shape[1:]
    wide = lons + (-lons % LANES)
    blocks, slots = obs_values.shape[1:]

    trade = []
    for i in range(count_l - 1):
        trade += [(2 * i + 1, 2 * i + 2), (2 * i + 2, 2 * i + 1)]
    band = LAT + ("ens",)
    partner = [(0, 1), (1, 0)]
    own = (HALF, levels, wide)
    quarter = (4, levels, wide)
    fields = (increment, wind_lon, wind_lat)
    piece = buf(levels, HALF, lons)
    whole = buf(levels, band_rows, lons)

    (outgoing,) = call(
        edge_kernel, [HBM] * 3, [(10, levels, wide)], [piece, piece, piece, pltpu.SemaphoreType.DMA((3,))]
    )(*(in_hbm(field) for field in fields))
    halo = lax.ppermute(outgoing, band, trade)
    own_rows, field = call(own_kernel, [VMEM], [own, (12, levels, wide)])(increment)
    next_rows = lax.ppermute(own_rows, TM, [(i + 1, i) for i in range(count_t - 1)])
    coefs, prec, weight = call(
        prepare_kernel,
        [HBM] * 2 + [SMEM] + [VMEM] * 3,
        [(5, 12, levels, wide), (levels, wide), (slots, blocks)],
        [whole, whole, pltpu.SemaphoreType.DMA((2,))],
    )(in_hbm(wind_lon), in_hbm(wind_lat), model_precision, obs_rows, obs_counts, obs_precision[0].T)
    other_pert = lax.ppermute(perturbations, "ens", partner)

    later, adj, outer, inner, edges = call(
        forward_kernel,
        [VMEM] * 5 + [HBM, HBM] + [VMEM] * 2,
        [own, own, quarter, quarter, (5, 4, levels, wide)],
        [
            buf(16, levels, wide), buf(16, levels, wide), buf(blocks, wide), buf(slots, blocks),
            buf(blocks, slots, lons), pltpu.SMEM((1, blocks), jnp.int32), pltpu.SemaphoreType.DMA((2,)),
        ],
    )(field, coefs, prec, halo, next_rows, in_hbm(obs_jacobian), in_hbm(obs_rows), obs_values[0].T, weight)
    outer = lax.ppermute(outer, band, trade)
    inner = lax.ppermute(inner, "ens", partner)
    mismatch = lax.ppermute(later, TM, [(i, i + 1) for i in range(count_t - 1)])

    forcing, start = call(
        adjoint_kernel,
        [VMEM] * 5,
        [(levels, HALF, lons), own],
        [buf(16, levels, wide), buf(16, levels, wide), buf(*own)],
    )(adj, outer, inner, edges, coefs)
    pieces = lax.all_to_all(forcing, TM, 0, 0, tiled=True)

    (products,) = call(product_kernel, [VMEM] * 3, [(count_t * count_l, 1, LANES)])(
        pieces, perturbations, other_pert
    )
    start, mismatch, products = lax.optimization_barrier((start, mismatch, products))
    (own_grad,) = call(mismatch_kernel, [VMEM] * 4, [own])(start, mismatch, own_rows, prec)
    other_grad = lax.ppermute(own_grad, "ens", partner)
    sums = lax.all_to_all(products, TM_LAT, 0, 0, tiled=True)
    (grad_state,) = call(gradient_kernel, [VMEM] * 2, [(1, levels, band_rows, lons)])(own_grad, other_grad)

    (total,) = call(sum_kernel, [VMEM], [(HALF, LANES)])(sums)
    other_total = lax.ppermute(total, "ens", partner)
    (forcing_step,) = call(step_kernel, [VMEM] * 4, [(1, band_rows, lons)])(
        total, other_total, perturbations, other_pert
    )
    return (grad_state, forcing_step)


def solution(mesh):
    torus = Mesh(
        mesh.devices.reshape(2, 4, 8, 2, mesh.shape["ens"]),
        ("tm_0", "tm_1", "lat_0", "lat_1", "ens"),
    )
    in_specs = (
        P(TM, None, LAT, None),
        P(TM, None, LAT, None),
        P(TM, None, LAT, None),
        P(),
        P("ens", TM, LAT, None),
        P(TM, LAT),
        P(TM, LAT, None, None),
        P(TM, LAT, None),
        P(TM, LAT, None),
        P(TM, LAT),
    )
    out_specs = (P(TM, None, LAT, None), P(TM, LAT, None))

    return jax.shard_map(on_device, mesh=torus, in_specs=in_specs, out_specs=out_specs, check_vma=False)
```

```python
import jax
import jax.numpy as jnp
from jax import lax
from jax.experimental import pallas as pl
from jax.experimental.pallas import tpu as pltpu
from jax.sharding import Mesh
from jax.sharding import PartitionSpec as P

MEM = 32
STEPS = 4
LANES = 128
HALF = 8
TM = ("tm_0", "tm_1")
LAT = ("lat_0", "lat_1")
TM_LAT = ("tm_0", "tm_1", "lat_0", "lat_1")


def east(value):
    return pltpu.roll(value, value.shape[-1] - 1, 1)


def west(value):
    return pltpu.roll(value, 1, 1)


def wrap(ref, lons):
    tail = lons % LANES
    half = (LANES - tail) // 2
    first = ref[:, 0:LANES]
    lane = lax.broadcasted_iota(jnp.int32, first.shape, 1)
    last = jnp.where(lane < tail, ref[:, lons - tail :], 0.0)
    ref[:, lons - tail :] = jnp.where(
        lane < tail, last, jnp.where(lane < tail + half, pltpu.roll(first, tail, 1), pltpu.roll(last, LANES - tail, 1))
    )


def fetch(source, first, size, target, sem):
    return pltpu.make_async_copy(source.at[0, :, pl.ds(first, size), :], target, sem)


def edge_kernel(inc_hbm, lon_hbm, lat_hbm, out_ref, inc, lon, lat, sems):
    core = lax.axis_index("ens")
    lons = inc.shape[-1]
    levels = inc.shape[0]

    def rows(first, at):
        copies = [
            fetch(source, first, HALF, target, sems.at[i])
            for i, (source, target) in enumerate(((inc_hbm, inc), (lon_hbm, lon), (lat_hbm, lat)))
        ]
        for copy in copies:
            copy.start()
        sign = 1.0 if at(0) == 7 else -1.0
        for i, copy in enumerate(copies):
            copy.wait()
            buf = (inc, lon, lat)[i]
            base = (0, 4, 7)[i]
            for q in range(4 if i == 0 else 3):
                r = 3 - q if i == 0 else 2 - q
                value = buf[:, at(r), :]
                if i == 2:
                    value = sign * value
                out_ref[base + q, :, 0:lons] = value
                wrap(out_ref.at[base + q], lons)

    @pl.when(core == 0)
    def _():
        rows(0, lambda r: r)

    @pl.when(core == 1)
    def _():
        rows(HALF, lambda r: 7 - r)


def own_kernel(inc_ref, own_ref, field_ref):
    core = lax.axis_index("ens")
    lons = inc_ref.shape[-1]

    def rows(at):
        for r in range(12):
            field_ref[r, :, 0:lons] = inc_ref[0, :, at(r), :]
            wrap(field_ref.at[r], lons)
            if r < HALF:
                own_ref[r] = field_ref[r]

    @pl.when(core == 0)
    def _():
        rows(lambda r: r)

    @pl.when(core == 1)
    def _():
        rows(lambda r: 15 - r)


class Rows:
    def __init__(self, halo_ref, own_ref, at):
        self.halo, self.own, self.at = halo_ref, own_ref, at

    def __getitem__(self, j):
        return self.halo[self.at, j] if j < 4 else self.own[self.at, j - 4]


def forward_step(src, dst, coefs, first, last):
    center, plon, mlon, plat, mlat = coefs
    for j in range(first, last):
        f = src[j]
        dst[j] = center[j] * f + plon[j] * east(f) + mlon[j] * west(f) + plat[j] * src[j + 1] + mlat[j] * src[j - 1]


def adjoint_step(src, dst, coefs, first, last):
    center, plon, mlon, plat, mlat = coefs
    for j in range(first, last):
        g = src[j]
        dst[j] = (
            center[j] * g
            + west(plon[j] * g)
            + east(mlon[j] * g)
            + plat[j - 1] * src[j - 1]
            + mlat[j + 1] * src[j + 1]
        )


def inner_steps(step_of, bufs, coefs, joint_ref, done):
    for s in range(1, STEPS + 1):
        src, dst = bufs[(s - 1) % 2], bufs[s % 2]
        step_of(src, dst, coefs, 4 + s, 16 - s)
        if s < STEPS:
            joint_ref[s - 1, 0] = dst[4 + s]
            joint_ref[s - 1, 1] = dst[5 + s]
        done(s, dst)


def outer_steps(step_of, bufs, coefs, joint_ref, done):
    for s in range(1, STEPS + 1):
        src, dst = bufs[(s - 1) % 2], bufs[s % 2]
        step_of(src, dst, coefs, s, 4 + s)
        if s < STEPS:
            dst[4 + s] = joint_ref[s - 1, 0]
            dst[5 + s] = joint_ref[s - 1, 1]
        done(s, dst)


def prepare_kernel(
    lon_hbm, lat_hbm, field_ref, prec_ref, rows_ref, counts_ref, oprec_ref,
    coef_ref, prec_out, weight_ref, joint_ref, end_ref, lon, lat, x0, x1, sems,
):
    core = lax.axis_index("ens")
    lons = lon.shape[-1]
    levels = lon.shape[0]
    copies = [
        fetch(source, 0, 2 * HALF, target, sems.at[i])
        for i, (source, target) in enumerate(((lon_hbm, lon), (lat_hbm, lat)))
    ]
    for copy in copies:
        copy.start()
    level = lax.broadcasted_iota(jnp.int32, prec_out.shape, 0)
    prec = jnp.zeros(prec_out.shape, jnp.float32)
    for k in range(levels):
        prec = jnp.where(level == k, prec_ref[k], prec)
    prec_out[...] = prec
    slot = lax.broadcasted_iota(jnp.int32, weight_ref.shape, 0)
    mine = (rows_ref[...] % 16) // HALF == core
    weight_ref[...] = jnp.where((slot < counts_ref[...]) & mine, oprec_ref[...], 0.0)
    for copy in copies:
        copy.wait()

    def rows(at, sign):
        for r in range(12):
            coef_ref[1, r, :, 0:lons] = lon[:, at(r), :]
            wrap(coef_ref.at[1, r], lons)
            coef_ref[4, r, :, 0:lons] = sign * lat[:, at(r), :]
            wrap(coef_ref.at[4, r], lons)
            store_coefficients(coef_ref, r, coef_ref[1, r], coef_ref[4, r])

    @pl.when(core == 0)
    def _():
        rows(lambda r: r, 1.0)

    @pl.when(core == 1)
    def _():
        rows(lambda r: 15 - r, -1.0)

    x0[4:16] = field_ref[...]
    coefs = [Rows(None, coef_ref, i) for i in range(5)]

    def done(step, dst):
        if step == STEPS:
            end_ref[...] = dst[8:12]

    inner_steps(forward_step, (x0, x1), coefs, joint_ref, done)


def store_coefficients(coef_ref, at, c, e):
    cc = c * c
    ee = e * e
    coef_ref[0, at] = 1.0 - cc - ee
    coef_ref[1, at] = 0.5 * (cc - c)
    coef_ref[2, at] = 0.5 * (cc + c)
    coef_ref[3, at] = 0.5 * (ee - e)
    coef_ref[4, at] = 0.5 * (ee + e)


def forward_kernel(
    field_ref, coef_ref, joint_ref, far_ref, halo_ref, jac_hbm, rows_hbm, val_ref, weight_ref,
    end_ref, force_ref, edge_ref, x0, x1, pk, wgt, jac, rows, sems,
):
    core = lax.axis_index("ens")
    blocks, slots, lons = jac.shape
    jac_copy = pltpu.make_async_copy(jac_hbm.at[0], jac, sems.at[0])
    rows_copy = pltpu.make_async_copy(rows_hbm, rows, sems.at[1])
    jac_copy.start()
    rows_copy.start()
    x0[0:4] = halo_ref[0:4]
    x0[4:6] = field_ref[0:2]
    edge_ref[3, 0] = jnp.ones(x0.shape[1:], jnp.float32)
    for r in range(3):
        store_coefficients(edge_ref, 1 + r, halo_ref[4 + r], halo_ref[7 + r])
    coefs = [Rows(edge_ref, coef_ref, i) for i in range(5)]

    def done(step, dst):
        if step == STEPS:
            end_ref[0:4] = dst[4:8]

    outer_steps(forward_step, (x0, x1), coefs, joint_ref, done)
    end_ref[4:8] = far_ref[...]
    force_ref[...] = jnp.zeros(force_ref.shape, jnp.float32)

    rows_copy.wait()
    jac_copy.wait()

    def place(j):
        r = rows[0, j]
        lat = r % 16
        row = jnp.clip(jnp.where(core == 0, lat, 15 - lat), 0, HALF - 1)
        return row, pl.ds(r // 16, 1)

    for j in range(blocks):
        row, lev = place(j)
        pk[pl.ds(j, 1), :] = end_ref[row, lev, :]
    lane = lax.broadcasted_iota(jnp.int32, (slots, blocks), 1)
    ev = jnp.zeros((slots, blocks), jnp.float32)
    for j in range(blocks):
        total = jnp.sum(jac[j] * pk[pl.ds(j, 1), 0:lons], axis=1, keepdims=True)
        ev = jnp.where(lane == j, total, ev)
    wgt[...] = weight_ref[...] * (ev - val_ref[...])
    for j in range(blocks):
        w = jnp.sum(jnp.where(lane == j, wgt[...], 0.0), axis=1, keepdims=True)
        pk[pl.ds(j, 1), 0:lons] = jnp.sum(jac[j] * w, axis=0, keepdims=True)
    wrap(pk, lons)
    for j in range(blocks):
        row, lev = place(j)
        force_ref[row, lev, :] = force_ref[row, lev, :] + pk[pl.ds(j, 1), :]


def seed_kernel(force_ref, end_ref, next_ref, prec_ref, coef_ref, later_ref, adj_ref, outer_ref, inner_ref):
    has_next = (lax.axis_index(TM) < lax.axis_size(TM) - 1).astype(jnp.float32)
    prec = prec_ref[...] * has_next
    for r in range(HALF):
        later = prec * (next_ref[r] - end_ref[r])
        later_ref[r] = later
        adj_ref[r] = force_ref[r] - later
    for q in range(4):
        outer_ref[q] = adj_ref[3 - q] * coef_ref[4, 3] if q == 0 else adj_ref[3 - q]
        inner_ref[q] = adj_ref[7 - q]


def adjoint_inner_kernel(adj_ref, inner_ref, coef_ref, joint_ref, far_ref, total_ref, g0, g1):
    g0[4:12] = adj_ref[...]
    g0[12:16] = inner_ref[...]
    coefs = [Rows(None, coef_ref, i) for i in range(5)]
    total_ref[...] = adj_ref[...]

    def done(step, dst):
        if step == STEPS:
            far_ref[...] = dst[8:12]
        else:
            for j in range(4 + step, 12):
                total_ref[j - 4] = total_ref[j - 4] + dst[j]

    inner_steps(adjoint_step, (g0, g1), coefs, joint_ref, done)


def adjoint_kernel(
    adj_ref, outer_ref, edge_ref, coef_ref, joint_ref, far_ref, total_ref, forcing_ref, start_ref, g0, g1, sums
):
    core = lax.axis_index("ens")
    lons = forcing_ref.shape[-1]
    g0[0:4] = outer_ref[...]
    g0[4:6] = adj_ref[0:2]
    coefs = [Rows(edge_ref, coef_ref, i) for i in range(5)]
    sums[...] = total_ref[0:3]
    start_ref[4:8] = far_ref[...]

    def done(step, dst):
        if step == STEPS:
            start_ref[0:4] = dst[4:8]
        else:
            for j in range(4, 4 + step):
                sums[j - 4] = sums[j - 4] + dst[j]

    outer_steps(adjoint_step, (g0, g1), coefs, joint_ref, done)

    def store(at):
        for r in range(HALF):
            forcing_ref[:, at(r), :] = (sums if r < 3 else total_ref)[r, :, 0:lons]

    @pl.when(core == 0)
    def _():
        store(lambda r: r)

    @pl.when(core == 1)
    def _():
        store(lambda r: 7 - r)


def mismatch_kernel(start_ref, mismatch_ref, inc_ref, prec_ref, grad_ref):
    first_window = lax.axis_index(TM) == 0
    prec = prec_ref[...]
    for r in range(HALF):
        grad_ref[r] = start_ref[r] + jnp.where(first_window, prec * inc_ref[r], mismatch_ref[r])


def product_kernel(pieces_ref, own_ref, other_ref, out_ref):
    core = lax.axis_index("ens")
    forcing = jnp.sum(pieces_ref[...], axis=0)
    lane = lax.broadcasted_iota(jnp.int32, (HALF, LANES), 1)
    members = own_ref.shape[0]
    first = pl.multiple_of(HALF * core, HALF)
    vec = jnp.zeros((HALF, LANES), jnp.float32)
    for m in range(2 * members):
        ref, at = (own_ref, m) if m < members else (other_ref, m - members)
        col = jnp.sum(ref[at, 0, pl.ds(first, HALF), :] * forcing, axis=1, keepdims=True)
        vec = jnp.where(lane == m, col, vec)
    vec = jnp.sum(vec, axis=0, keepdims=True)
    out_ref[...] = jnp.broadcast_to(vec[None], out_ref.shape)


def sum_kernel(sums_ref, out_ref):
    vec = jnp.sum(sums_ref[...], axis=0)
    out_ref[...] = jnp.broadcast_to(vec, out_ref.shape)


def step_kernel(sum_ref, other_sum_ref, own_ref, other_ref, out_ref):
    members = own_ref.shape[0]
    lane = lax.broadcasted_iota(jnp.int32, (HALF, LANES), 1)
    theirs = other_sum_ref[...]
    swapped = jnp.where(
        lane < members, pltpu.roll(theirs, LANES - members, 1), pltpu.roll(theirs, members, 1)
    )
    vec = (sum_ref[...] + swapped) * (-1.0 / (MEM - 1.0))
    coefs = [jnp.sum(jnp.where(lane == m, vec, 0.0), axis=1, keepdims=True) for m in range(2 * members)]
    for half in range(2):
        rows = pl.ds(HALF * half, HALF)
        total = coefs[0] * own_ref[0, 0, rows, :]
        for m in range(1, 2 * members):
            ref, at = (own_ref, m) if m < members else (other_ref, m - members)
            total = total + coefs[m] * ref[at, 0, rows, :]
        out_ref[0, rows, :] = total


def gradient_kernel(own_ref, other_ref, out_ref):
    core = lax.axis_index("ens")
    lons = out_ref.shape[-1]

    def store(north, south):
        for r in range(HALF):
            out_ref[0, :, r, :] = north[r, :, 0:lons]
            out_ref[0, :, 15 - r, :] = south[r, :, 0:lons]

    @pl.when(core == 0)
    def _():
        store(own_ref, other_ref)

    @pl.when(core == 1)
    def _():
        store(other_ref, own_ref)


VMEM = pl.BlockSpec(memory_space=pltpu.VMEM)
SMEM = pl.BlockSpec(memory_space=pltpu.SMEM)
HBM = pl.BlockSpec(memory_space=pltpu.HBM)


def buf(*shape):
    return pltpu.VMEM(shape, jnp.float32)


def in_hbm(value):
    return pltpu.with_memory_space_constraint(value, pltpu.HBM)


def call(kernel, ins, outs, scratch=(), limit=40):
    return pl.pallas_call(
        kernel,
        out_shape=[jax.ShapeDtypeStruct(s, jnp.float32) for s in outs],
        in_specs=ins,
        out_specs=[VMEM] * len(outs),
        scratch_shapes=list(scratch),
        compiler_params=pltpu.CompilerParams(vmem_limit_bytes=int(limit * 2**20)),
    )


def on_device(
    increment,
    wind_lon,
    wind_lat,
    model_precision,
    perturbations,
    obs_rows,
    obs_jacobian,
    obs_values,
    obs_precision,
    obs_counts,
):
    count_t = lax.axis_size(TM)
    count_l = lax.axis_size(LAT)
    levels, band_rows, lons = increment.shape[1:]
    wide = lons + (-lons % LANES)
    blocks, slots = obs_values.shape[1:]

    trade = []
    for i in range(count_l - 1):
        trade += [(2 * i + 1, 2 * i + 2), (2 * i + 2, 2 * i + 1)]
    band = LAT + ("ens",)
    partner = [(0, 1), (1, 0)]
    own = (HALF, levels, wide)
    quarter = (4, levels, wide)
    fields = (increment, wind_lon, wind_lat)
    piece = buf(levels, HALF, lons)
    whole = buf(levels, band_rows, lons)

    (outgoing,) = call(
        edge_kernel, [HBM] * 3, [(10, levels, wide)], [piece, piece, piece, pltpu.SemaphoreType.DMA((3,))]
    )(*(in_hbm(field) for field in fields))
    halo = lax.ppermute(outgoing, band, trade)
    own_rows, field = call(own_kernel, [VMEM], [own, (12, levels, wide)])(increment)
    next_rows = lax.ppermute(own_rows, TM, [(i + 1, i) for i in range(count_t - 1)])
    working = buf(16, levels, wide)
    joint = (STEPS - 1, 2, levels, wide)
    coefs, prec, weight, joint_rows, far = call(
        prepare_kernel,
        [HBM] * 2 + [VMEM, SMEM] + [VMEM] * 3,
        [(5, 12, levels, wide), (levels, wide), (slots, blocks), joint, quarter],
        [whole, whole, working, working, pltpu.SemaphoreType.DMA((2,))],
    )(in_hbm(wind_lon), in_hbm(wind_lat), field, model_precision, obs_rows, obs_counts, obs_precision[0].T)
    other_pert = lax.ppermute(perturbations, "ens", partner)

    end, force, edges = call(
        forward_kernel,
        [VMEM] * 5 + [HBM, HBM] + [VMEM] * 2,
        [own, own, (5, 4, levels, wide)],
        [
            working, working, buf(blocks, wide), buf(slots, blocks),
            buf(blocks, slots, lons), pltpu.SMEM((1, blocks), jnp.int32), pltpu.SemaphoreType.DMA((2,)),
        ],
    )(field, coefs, joint_rows, far, halo, in_hbm(obs_jacobian), in_hbm(obs_rows), obs_values[0].T, weight)
    next_rows, end = lax.optimization_barrier((next_rows, end))
    later, adj, outer, inner = call(seed_kernel, [VMEM] * 5, [own, own, quarter, quarter])(
        force, end, next_rows, prec, coefs
    )
    outer = lax.ppermute(outer, band, trade)
    inner = lax.ppermute(inner, "ens", partner)
    mismatch = lax.ppermute(later, TM, [(i, i + 1) for i in range(count_t - 1)])

    joint_rows, far, total = call(
        adjoint_inner_kernel, [VMEM] * 3, [joint, quarter, own], [working, working]
    )(adj, inner, coefs)
    forcing, start = call(
        adjoint_kernel,
        [VMEM] * 7,
        [(levels, HALF, lons), own],
        [working, working, buf(3, levels, wide)],
    )(adj, outer, edges, coefs, joint_rows, far, total)
    pieces = lax.all_to_all(forcing, TM, 0, 0, tiled=True)

    (products,) = call(product_kernel, [VMEM] * 3, [(count_t * count_l, 1, LANES)])(
        pieces, perturbations, other_pert
    )
    start, mismatch, products = lax.optimization_barrier((start, mismatch, products))
    (own_grad,) = call(mismatch_kernel, [VMEM] * 4, [own])(start, mismatch, own_rows, prec)
    other_grad = lax.ppermute(own_grad, "ens", partner)
    sums = lax.all_to_all(products, TM_LAT, 0, 0, tiled=True)
    (grad_state,) = call(gradient_kernel, [VMEM] * 2, [(1, levels, band_rows, lons)])(own_grad, other_grad)

    (total,) = call(sum_kernel, [VMEM], [(HALF, LANES)])(sums)
    other_total = lax.ppermute(total, "ens", partner)
    (forcing_step,) = call(step_kernel, [VMEM] * 4, [(1, band_rows, lons)])(
        total, other_total, perturbations, other_pert
    )
    return (grad_state, forcing_step)


def solution(mesh):
    torus = Mesh(
        mesh.devices.reshape(2, 4, 8, 2, mesh.shape["ens"]),
        ("tm_0", "tm_1", "lat_0", "lat_1", "ens"),
    )
    in_specs = (
        P(TM, None, LAT, None),
        P(TM, None, LAT, None),
        P(TM, None, LAT, None),
        P(),
        P("ens", TM, LAT, None),
        P(TM, LAT),
        P(TM, LAT, None, None),
        P(TM, LAT, None),
        P(TM, LAT, None),
        P(TM, LAT),
    )
    out_specs = (P(TM, None, LAT, None), P(TM, LAT, None))

    return jax.shard_map(on_device, mesh=torus, in_specs=in_specs, out_specs=out_specs, check_vma=False)
```

```python
import jax
import jax.numpy as jnp
from jax import lax
from jax.experimental import pallas as pl
from jax.experimental.pallas import tpu as pltpu
from jax.sharding import Mesh
from jax.sharding import PartitionSpec as P

MEM = 32
STEPS = 4
LANES = 128
HALF = 8
TM = ("tm_0", "tm_1")
LAT = ("lat_0", "lat_1")
TM_LAT = ("tm_0", "tm_1", "lat_0", "lat_1")


def east(value):
    return pltpu.roll(value, value.shape[-1] - 1, 1)


def west(value):
    return pltpu.roll(value, 1, 1)


def wrap(ref, lons):
    tail = lons % LANES
    half = (LANES - tail) // 2
    first = ref[:, 0:LANES]
    lane = lax.broadcasted_iota(jnp.int32, first.shape, 1)
    last = jnp.where(lane < tail, ref[:, lons - tail :], 0.0)
    ref[:, lons - tail :] = jnp.where(
        lane < tail, last, jnp.where(lane < tail + half, pltpu.roll(first, tail, 1), pltpu.roll(last, LANES - tail, 1))
    )


def fetch(source, first, size, target, sem):
    return pltpu.make_async_copy(source.at[0, :, pl.ds(first, size), :], target, sem)


def edge_kernel(inc_hbm, lon_hbm, lat_hbm, out_ref, inc, lon, lat, sems):
    core = lax.axis_index("ens")
    lons = inc.shape[-1]
    levels = inc.shape[0]

    def rows(first, at):
        copies = [
            fetch(source, first, HALF, target, sems.at[i])
            for i, (source, target) in enumerate(((inc_hbm, inc), (lon_hbm, lon), (lat_hbm, lat)))
        ]
        for copy in copies:
            copy.start()
        sign = 1.0 if at(0) == 7 else -1.0
        for i, copy in enumerate(copies):
            copy.wait()
            buf = (inc, lon, lat)[i]
            base = (0, 4, 7)[i]
            for q in range(4 if i == 0 else 3):
                r = 3 - q if i == 0 else 2 - q
                value = buf[:, at(r), :]
                if i == 2:
                    value = sign * value
                out_ref[base + q, :, 0:lons] = value
                wrap(out_ref.at[base + q], lons)

    @pl.when(core == 0)
    def _():
        rows(0, lambda r: r)

    @pl.when(core == 1)
    def _():
        rows(HALF, lambda r: 7 - r)


def own_kernel(inc_ref, near_ref, far_ref, field_ref):
    core = lax.axis_index("ens")
    lons = inc_ref.shape[-1]

    def rows(at):
        for r in range(12):
            field_ref[r, :, 0:lons] = inc_ref[0, :, at(r), :]
            wrap(field_ref.at[r], lons)
            if r < HALF:
                (near_ref if r < 4 else far_ref)[r % 4] = field_ref[r]

    @pl.when(core == 0)
    def _():
        rows(lambda r: r)

    @pl.when(core == 1)
    def _():
        rows(lambda r: 15 - r)


class Rows:
    def __init__(self, halo_ref, own_ref, at):
        self.halo, self.own, self.at = halo_ref, own_ref, at

    def __getitem__(self, j):
        return self.halo[self.at, j] if j < 4 else self.own[self.at, j - 4]


def forward_step(src, dst, coefs, first, last):
    center, plon, mlon, plat, mlat = coefs
    for j in range(first, last):
        f = src[j]
        dst[j] = center[j] * f + plon[j] * east(f) + mlon[j] * west(f) + plat[j] * src[j + 1] + mlat[j] * src[j - 1]


def adjoint_step(src, dst, coefs, first, last):
    center, plon, mlon, plat, mlat = coefs
    for j in range(first, last):
        g = src[j]
        dst[j] = (
            center[j] * g
            + west(plon[j] * g)
            + east(mlon[j] * g)
            + plat[j - 1] * src[j - 1]
            + mlat[j + 1] * src[j + 1]
        )


def inner_steps(step_of, bufs, coefs, joint_ref, done):
    for s in range(1, STEPS + 1):
        src, dst = bufs[(s - 1) % 2], bufs[s % 2]
        step_of(src, dst, coefs, 4 + s, 16 - s)
        if s < STEPS:
            joint_ref[s - 1, 0] = dst[4 + s]
            joint_ref[s - 1, 1] = dst[5 + s]
        done(s, dst)


def outer_steps(step_of, bufs, coefs, joint_ref, done):
    for s in range(1, STEPS + 1):
        src, dst = bufs[(s - 1) % 2], bufs[s % 2]
        step_of(src, dst, coefs, s, 4 + s)
        if s < STEPS:
            dst[4 + s] = joint_ref[s - 1, 0]
            dst[5 + s] = joint_ref[s - 1, 1]
        done(s, dst)


def prepare_kernel(
    lon_hbm, lat_hbm, jac_hbm, field_ref, prec_ref, rows_ref, counts_ref, oprec_ref,
    coef_ref, prec_out, weight_ref, joint_ref, end_ref, jac_ref, lon, lat, x0, x1, sems,
):
    core = lax.axis_index("ens")
    lons = lon.shape[-1]
    levels = lon.shape[0]
    copies = [
        fetch(source, 0, 2 * HALF, target, sems.at[i])
        for i, (source, target) in enumerate(((lon_hbm, lon), (lat_hbm, lat)))
    ]
    for copy in copies:
        copy.start()
    jac_copy = pltpu.make_async_copy(jac_hbm.at[0], jac_ref, sems.at[2])
    jac_copy.start()
    level = lax.broadcasted_iota(jnp.int32, prec_out.shape, 0)
    prec = jnp.zeros(prec_out.shape, jnp.float32)
    for k in range(levels):
        prec = jnp.where(level == k, prec_ref[k], prec)
    prec_out[...] = prec
    slot = lax.broadcasted_iota(jnp.int32, weight_ref.shape, 0)
    mine = (rows_ref[...] % 16) // HALF == core
    weight_ref[...] = jnp.where((slot < counts_ref[...]) & mine, oprec_ref[...], 0.0)
    for copy in copies:
        copy.wait()

    def rows(at, sign):
        for r in range(12):
            coef_ref[1, r, :, 0:lons] = lon[:, at(r), :]
            wrap(coef_ref.at[1, r], lons)
            coef_ref[4, r, :, 0:lons] = sign * lat[:, at(r), :]
            wrap(coef_ref.at[4, r], lons)
            store_coefficients(coef_ref, r, coef_ref[1, r], coef_ref[4, r])

    @pl.when(core == 0)
    def _():
        rows(lambda r: r, 1.0)

    @pl.when(core == 1)
    def _():
        rows(lambda r: 15 - r, -1.0)

    x0[4:16] = field_ref[...]
    coefs = [Rows(None, coef_ref, i) for i in range(5)]

    def done(step, dst):
        if step == STEPS:
            end_ref[...] = dst[8:12]

    inner_steps(forward_step, (x0, x1), coefs, joint_ref, done)
    jac_copy.wait()


def store_coefficients(coef_ref, at, c, e):
    cc = c * c
    ee = e * e
    coef_ref[0, at] = 1.0 - cc - ee
    coef_ref[1, at] = 0.5 * (cc - c)
    coef_ref[2, at] = 0.5 * (cc + c)
    coef_ref[3, at] = 0.5 * (ee - e)
    coef_ref[4, at] = 0.5 * (ee + e)


def forward_kernel(
    field_ref, coef_ref, joint_ref, far_ref, halo_ref, jac, rows_hbm, val_ref, weight_ref,
    end_ref, force_ref, edge_ref, x0, x1, pk, wgt, rows, sem,
):
    core = lax.axis_index("ens")
    blocks, slots, lons = jac.shape
    rows_copy = pltpu.make_async_copy(rows_hbm, rows, sem)
    rows_copy.start()
    x0[0:4] = halo_ref[0:4]
    x0[4:6] = field_ref[0:2]
    edge_ref[3, 0] = jnp.ones(x0.shape[1:], jnp.float32)
    for r in range(3):
        store_coefficients(edge_ref, 1 + r, halo_ref[4 + r], halo_ref[7 + r])
    coefs = [Rows(edge_ref, coef_ref, i) for i in range(5)]

    def done(step, dst):
        if step == STEPS:
            end_ref[...] = dst[4:8]
            dst[8:12] = far_ref[...]

    outer_steps(forward_step, (x0, x1), coefs, joint_ref, done)
    field = (x0, x1)[STEPS % 2]
    force_ref[...] = jnp.zeros(force_ref.shape, jnp.float32)

    rows_copy.wait()

    def place(j):
        r = rows[0, j]
        lat = r % 16
        row = jnp.clip(jnp.where(core == 0, lat, 15 - lat), 0, HALF - 1)
        return row, pl.ds(r // 16, 1)

    for j in range(blocks):
        row, lev = place(j)
        pk[pl.ds(j, 1), :] = field[4 + row, lev, :]
    lane = lax.broadcasted_iota(jnp.int32, (slots, blocks), 1)
    ev = jnp.zeros((slots, blocks), jnp.float32)
    for j in range(blocks):
        total = jnp.sum(jac[j] * pk[pl.ds(j, 1), 0:lons], axis=1, keepdims=True)
        ev = jnp.where(lane == j, total, ev)
    wgt[...] = weight_ref[...] * (ev - val_ref[...])
    for j in range(blocks):
        w = jnp.sum(jnp.where(lane == j, wgt[...], 0.0), axis=1, keepdims=True)
        pk[pl.ds(j, 1), 0:lons] = jnp.sum(jac[j] * w, axis=0, keepdims=True)
    wrap(pk, lons)
    for j in range(blocks):
        row, lev = place(j)
        force_ref[row, lev, :] = force_ref[row, lev, :] + pk[pl.ds(j, 1), :]


def with_next():
    return (lax.axis_index(TM) < lax.axis_size(TM) - 1).astype(jnp.float32)


def near_kernel(force_ref, end_ref, next_ref, prec_ref, coef_ref, adj_ref, outer_ref):
    prec = prec_ref[...] * with_next()
    for r in range(4):
        adj = force_ref[r] - prec * (next_ref[r] - end_ref[r])
        adj_ref[r] = adj
        outer_ref[3 - r] = adj * coef_ref[4, 3] if r == 3 else adj


def far_kernel(force_ref, end_ref, next_ref, prec_ref, adj_ref, inner_ref):
    prec = prec_ref[...] * with_next()
    for r in range(4):
        adj = force_ref[4 + r] - prec * (next_ref[r] - end_ref[r])
        adj_ref[r] = adj
        inner_ref[3 - r] = adj


def adjoint_inner_kernel(near_ref, adj_ref, inner_ref, coef_ref, joint_ref, far_ref, total_ref, g0, g1):
    g0[4:8] = near_ref[...]
    g0[8:12] = adj_ref[...]
    g0[12:16] = inner_ref[...]
    coefs = [Rows(None, coef_ref, i) for i in range(5)]
    total_ref[0:4] = near_ref[...]
    total_ref[4:8] = adj_ref[...]

    def done(step, dst):
        if step == STEPS:
            far_ref[...] = dst[8:12]
        else:
            for j in range(4 + step, 12):
                total_ref[j - 4] = total_ref[j - 4] + dst[j]

    inner_steps(adjoint_step, (g0, g1), coefs, joint_ref, done)


def adjoint_kernel(
    adj_ref, outer_ref, edge_ref, coef_ref, joint_ref, far_ref, total_ref, forcing_ref, start_ref, g0, g1, sums
):
    core = lax.axis_index("ens")
    lons = forcing_ref.shape[-1]
    g0[0:4] = outer_ref[...]
    g0[4:6] = adj_ref[0:2]
    coefs = [Rows(edge_ref, coef_ref, i) for i in range(5)]
    sums[...] = total_ref[0:3]
    start_ref[4:8] = far_ref[...]

    def done(step, dst):
        if step == STEPS:
            start_ref[0:4] = dst[4:8]
        else:
            for j in range(4, 4 + step):
                sums[j - 4] = sums[j - 4] + dst[j]

    outer_steps(adjoint_step, (g0, g1), coefs, joint_ref, done)

    def store(at):
        for r in range(HALF):
            forcing_ref[:, at(r), :] = (sums if r < 3 else total_ref)[r, :, 0:lons]

    @pl.when(core == 0)
    def _():
        store(lambda r: r)

    @pl.when(core == 1)
    def _():
        store(lambda r: 7 - r)


def mismatch_kernel(start_ref, near_prior_ref, far_prior_ref, near_ref, far_ref, prec_ref, grad_ref):
    prec = prec_ref[...]
    for r in range(4):
        grad_ref[r] = start_ref[r] + prec * (near_ref[r] - near_prior_ref[r])
        grad_ref[4 + r] = start_ref[4 + r] + prec * (far_ref[r] - far_prior_ref[r])


def product_kernel(pieces_ref, own_ref, other_ref, out_ref):
    core = lax.axis_index("ens")
    forcing = jnp.sum(pieces_ref[...], axis=0)
    lane = lax.broadcasted_iota(jnp.int32, (HALF, LANES), 1)
    members = own_ref.shape[0]
    first = pl.multiple_of(HALF * core, HALF)
    vec = jnp.zeros((HALF, LANES), jnp.float32)
    for m in range(2 * members):
        ref, at = (own_ref, m) if m < members else (other_ref, m - members)
        col = jnp.sum(ref[at, 0, pl.ds(first, HALF), :] * forcing, axis=1, keepdims=True)
        vec = jnp.where(lane == m, col, vec)
    vec = jnp.sum(vec, axis=0, keepdims=True)
    out_ref[...] = jnp.broadcast_to(vec[None], out_ref.shape)


def sum_kernel(sums_ref, out_ref):
    vec = jnp.sum(sums_ref[...], axis=0)
    out_ref[...] = jnp.broadcast_to(vec, out_ref.shape)


def final_kernel(sum_ref, other_sum_ref, own_ref, other_ref, own_grad_ref, other_grad_ref, out_ref, grad_ref):
    store_gradient(own_grad_ref, other_grad_ref, grad_ref)
    members = own_ref.shape[0]
    lane = lax.broadcasted_iota(jnp.int32, (HALF, LANES), 1)
    theirs = other_sum_ref[...]
    swapped = jnp.where(
        lane < members, pltpu.roll(theirs, LANES - members, 1), pltpu.roll(theirs, members, 1)
    )
    vec = (sum_ref[...] + swapped) * (-1.0 / (MEM - 1.0))
    coefs = [jnp.sum(jnp.where(lane == m, vec, 0.0), axis=1, keepdims=True) for m in range(2 * members)]
    for half in range(2):
        rows = pl.ds(HALF * half, HALF)
        total = coefs[0] * own_ref[0, 0, rows, :]
        for m in range(1, 2 * members):
            ref, at = (own_ref, m) if m < members else (other_ref, m - members)
            total = total + coefs[m] * ref[at, 0, rows, :]
        out_ref[0, rows, :] = total


def store_gradient(own_ref, other_ref, out_ref):
    core = lax.axis_index("ens")
    lons = out_ref.shape[-1]

    def store(north, south):
        for r in range(HALF):
            out_ref[0, :, r, :] = north[r, :, 0:lons]
            out_ref[0, :, 15 - r, :] = south[r, :, 0:lons]

    @pl.when(core == 0)
    def _():
        store(own_ref, other_ref)

    @pl.when(core == 1)
    def _():
        store(other_ref, own_ref)


VMEM = pl.BlockSpec(memory_space=pltpu.VMEM)
SMEM = pl.BlockSpec(memory_space=pltpu.SMEM)
HBM = pl.BlockSpec(memory_space=pltpu.HBM)


def buf(*shape):
    return pltpu.VMEM(shape, jnp.float32)


def in_hbm(value):
    return pltpu.with_memory_space_constraint(value, pltpu.HBM)


def call(kernel, ins, outs, scratch=(), limit=40):
    return pl.pallas_call(
        kernel,
        out_shape=[jax.ShapeDtypeStruct(s, jnp.float32) for s in outs],
        in_specs=ins,
        out_specs=[VMEM] * len(outs),
        scratch_shapes=list(scratch),
        compiler_params=pltpu.CompilerParams(vmem_limit_bytes=int(limit * 2**20)),
    )


def on_device(
    increment,
    wind_lon,
    wind_lat,
    model_precision,
    perturbations,
    obs_rows,
    obs_jacobian,
    obs_values,
    obs_precision,
    obs_counts,
):
    count_t = lax.axis_size(TM)
    count_l = lax.axis_size(LAT)
    levels, band_rows, lons = increment.shape[1:]
    wide = lons + (-lons % LANES)
    blocks, slots = obs_values.shape[1:]

    trade = []
    for i in range(count_l - 1):
        trade += [(2 * i + 1, 2 * i + 2), (2 * i + 2, 2 * i + 1)]
    band = LAT + ("ens",)
    partner = [(0, 1), (1, 0)]
    own = (HALF, levels, wide)
    quarter = (4, levels, wide)
    fields = (increment, wind_lon, wind_lat)
    piece = buf(levels, HALF, lons)
    whole = buf(levels, band_rows, lons)

    (outgoing,) = call(
        edge_kernel, [HBM] * 3, [(10, levels, wide)], [piece, piece, piece, pltpu.SemaphoreType.DMA((3,))]
    )(*(in_hbm(field) for field in fields))
    halo = lax.ppermute(outgoing, band, trade)
    near_rows, far_rows, field = call(own_kernel, [VMEM], [quarter, quarter, (12, levels, wide)])(increment)
    earlier = [(i + 1, i) for i in range(count_t - 1)]
    next_near = lax.ppermute(near_rows, TM, earlier)
    next_far = lax.ppermute(far_rows, TM, earlier)
    working = buf(16, levels, wide)
    joint = (STEPS - 1, 2, levels, wide)
    coefs, prec, weight, joint_rows, far, jacobian = call(
        prepare_kernel,
        [HBM] * 3 + [VMEM, SMEM] + [VMEM] * 3,
        [(5, 12, levels, wide), (levels, wide), (slots, blocks), joint, quarter, (blocks, slots, lons)],
        [whole, whole, working, working, pltpu.SemaphoreType.DMA((3,))],
    )(in_hbm(wind_lon), in_hbm(wind_lat), in_hbm(obs_jacobian), field, model_precision, obs_rows, obs_counts, obs_precision[0].T)
    other_pert = lax.ppermute(perturbations, "ens", partner)

    later = [(i, i + 1) for i in range(count_t - 1)]
    far_prior = lax.ppermute(far, TM, later)
    end, force, edges = call(
        forward_kernel,
        [VMEM] * 6 + [HBM] + [VMEM] * 2,
        [quarter, own, (5, 4, levels, wide)],
        [
            working, working, buf(blocks, wide), buf(slots, blocks),
            pltpu.SMEM((1, blocks), jnp.int32), pltpu.SemaphoreType.DMA,
        ],
    )(field, coefs, joint_rows, far, halo, jacobian, in_hbm(obs_rows), obs_values[0].T, weight)
    near, outer = call(near_kernel, [VMEM] * 5, [quarter, quarter])(force, end, next_near, prec, coefs)
    outer = lax.ppermute(outer, band, trade)
    adj, inner = call(far_kernel, [VMEM] * 4, [quarter, quarter])(force, far, next_far, prec)
    inner = lax.ppermute(inner, "ens", partner)
    near_prior = lax.ppermute(end, TM, later)
    joint_rows, far_start, total = call(
        adjoint_inner_kernel, [VMEM] * 4, [joint, quarter, own], [working, working]
    )(near, adj, inner, coefs)
    forcing, start = call(
        adjoint_kernel,
        [VMEM] * 7,
        [(levels, HALF, lons), own],
        [working, working, buf(3, levels, wide)],
    )(near, outer, edges, coefs, joint_rows, far_start, total)
    pieces = lax.all_to_all(forcing, TM, 0, 0, tiled=True)

    (products,) = call(product_kernel, [VMEM] * 3, [(count_t * count_l, 1, LANES)])(
        pieces, perturbations, other_pert
    )
    start, near_prior, products = lax.optimization_barrier((start, near_prior, products))
    (own_grad,) = call(mismatch_kernel, [VMEM] * 6, [own])(start, near_prior, far_prior, near_rows, far_rows, prec)
    other_grad = lax.ppermute(own_grad, "ens", partner)
    sums = lax.all_to_all(products, TM_LAT, 0, 0, tiled=True)
    (total,) = call(sum_kernel, [VMEM], [(HALF, LANES)])(sums)
    other_total = lax.ppermute(total, "ens", partner)
    forcing_step, grad_state = call(
        final_kernel, [VMEM] * 6, [(1, band_rows, lons), (1, levels, band_rows, lons)]
    )(total, other_total, perturbations, other_pert, own_grad, other_grad)
    return (grad_state, forcing_step)


def solution(mesh):
    torus = Mesh(
        mesh.devices.reshape(2, 4, 8, 2, mesh.shape["ens"]),
        ("tm_0", "tm_1", "lat_0", "lat_1", "ens"),
    )
    in_specs = (
        P(TM, None, LAT, None),
        P(TM, None, LAT, None),
        P(TM, None, LAT, None),
        P(),
        P("ens", TM, LAT, None),
        P(TM, LAT),
        P(TM, LAT, None, None),
        P(TM, LAT, None),
        P(TM, LAT, None),
        P(TM, LAT),
    )
    out_specs = (P(TM, None, LAT, None), P(TM, LAT, None))

    return jax.shard_map(on_device, mesh=torus, in_specs=in_specs, out_specs=out_specs, check_vma=False)
```

```python
import jax
import jax.numpy as jnp
from jax import lax
from jax.experimental import pallas as pl
from jax.experimental.pallas import tpu as pltpu
from jax.sharding import Mesh
from jax.sharding import PartitionSpec as P

MEM = 32
STEPS = 4
LANES = 128
HALF = 8
TM = ("tm_0", "tm_1")
LAT = ("lat_0", "lat_1")
TM_LAT = ("tm_0", "tm_1", "lat_0", "lat_1")


def east(value):
    return pltpu.roll(value, value.shape[-1] - 1, 1)


def west(value):
    return pltpu.roll(value, 1, 1)


def wrap(ref, lons):
    tail = lons % LANES
    half = (LANES - tail) // 2
    first = ref[:, 0:LANES]
    lane = lax.broadcasted_iota(jnp.int32, first.shape, 1)
    last = jnp.where(lane < tail, ref[:, lons - tail :], 0.0)
    ref[:, lons - tail :] = jnp.where(
        lane < tail, last, jnp.where(lane < tail + half, pltpu.roll(first, tail, 1), pltpu.roll(last, LANES - tail, 1))
    )


def fetch(source, first, size, target, sem):
    return pltpu.make_async_copy(source.at[0, :, pl.ds(first, size), :], target, sem)


def edge_kernel(inc_hbm, lon_hbm, lat_hbm, out_ref, inc, lon, lat, x0, x1, coef, sems):
    core = lax.axis_index("ens")
    lons = inc.shape[-1]

    def rows(first, at, sign):
        copies = [
            fetch(source, first, HALF, target, sems.at[i])
            for i, (source, target) in enumerate(((inc_hbm, inc), (lon_hbm, lon), (lat_hbm, lat)))
        ]
        for copy in copies:
            copy.start()
        copies[0].wait()
        for r in range(4):
            x0[r, :, 0:lons] = inc[:, at(r), :]
            wrap(x0.at[r], lons)
        copies[1].wait()
        copies[2].wait()
        for r in range(3):
            coef[1, r, :, 0:lons] = lon[:, at(r), :]
            wrap(coef.at[1, r], lons)
            coef[4, r, :, 0:lons] = sign * lat[:, at(r), :]
            wrap(coef.at[4, r], lons)
            c, e = coef[1, r], coef[4, r]
            if r == 0:
                out_ref[4] = c
                out_ref[5] = -e
            if r == 1:
                out_ref[6] = -e
            store_coefficients(coef, r, c, e)
        out_ref[0] = x0[0]
        for s in range(1, STEPS):
            src, dst = (x0, x1) if s % 2 else (x1, x0)
            for r in range(4 - s):
                f = src[r]
                value = coef[0, r] * f + coef[1, r] * east(f) + coef[2, r] * west(f) + coef[3, r] * src[r + 1]
                dst[r] = value + coef[4, r] * src[r - 1] if r else value
            out_ref[s] = dst[0]

    @pl.when(core == 0)
    def _():
        rows(0, lambda r: r, 1.0)

    @pl.when(core == 1)
    def _():
        rows(HALF, lambda r: 7 - r, -1.0)


def own_kernel(inc_ref, near_ref, far_ref, field_ref):
    core = lax.axis_index("ens")
    lons = inc_ref.shape[-1]

    def rows(at):
        for r in range(12):
            field_ref[r, :, 0:lons] = inc_ref[0, :, at(r), :]
            wrap(field_ref.at[r], lons)
            if r < HALF:
                (near_ref if r < 4 else far_ref)[r % 4] = field_ref[r]

    @pl.when(core == 0)
    def _():
        rows(lambda r: r)

    @pl.when(core == 1)
    def _():
        rows(lambda r: 15 - r)


class Rows:
    def __init__(self, halo_ref, own_ref, at):
        self.halo, self.own, self.at = halo_ref, own_ref, at

    def __getitem__(self, j):
        return self.halo[self.at, j - 2] if j < 4 else self.own[self.at, j - 4]


def forward_step(src, dst, coefs, first, last):
    center, plon, mlon, plat, mlat = coefs
    for j in range(first, last):
        f = src[j]
        dst[j] = center[j] * f + plon[j] * east(f) + mlon[j] * west(f) + plat[j] * src[j + 1] + mlat[j] * src[j - 1]


def adjoint_step(src, dst, coefs, first, last):
    center, plon, mlon, plat, mlat = coefs
    for j in range(first, last):
        g = src[j]
        dst[j] = (
            center[j] * g
            + west(plon[j] * g)
            + east(mlon[j] * g)
            + plat[j - 1] * src[j - 1]
            + mlat[j + 1] * src[j + 1]
        )


def inner_steps(step_of, bufs, coefs, joint_ref, done):
    for s in range(1, STEPS + 1):
        src, dst = bufs[(s - 1) % 2], bufs[s % 2]
        step_of(src, dst, coefs, 4 + s, 16 - s)
        if s < STEPS:
            joint_ref[s - 1, 0] = dst[4 + s]
            joint_ref[s - 1, 1] = dst[5 + s]
        done(s, dst)


def outer_forward(bufs, coefs, joint_ref, halo_ref):
    center, plon, mlon, plat, mlat = coefs
    behind = rest = None
    for s in range(1, STEPS + 1):
        src, dst = bufs[(s - 1) % 2], bufs[s % 2]
        forward_step(src, dst, coefs, 4, 4 + s)
        if s < STEPS:
            dst[4 + s] = joint_ref[s - 1, 0]
            dst[5 + s] = joint_ref[s - 1, 1]
            value = plat[3] * src[4]
            if s > 1:
                value = value + center[3] * rest + plon[3] * east(rest) + mlon[3] * west(rest)
            if s > 2:
                value = value + mlat[3] * behind
            behind = plat[2] * rest if s > 1 else None
            rest = value
            dst[3] = halo_ref[s] + rest


def outer_adjoint(bufs, coefs, joint_ref, flux_ref, done):
    center, plon, mlon, plat, mlat = coefs
    behind = rest = None
    for s in range(1, STEPS + 1):
        src, dst = bufs[(s - 1) % 2], bufs[s % 2]
        g = src[4]
        flux = flux_ref[s - 1] if s == 1 else flux_ref[s - 1] + plat[3] * rest
        dst[4] = center[4] * g + west(plon[4] * g) + east(mlon[4] * g) + flux + mlat[5] * src[5]
        adjoint_step(src, dst, coefs, 5, 4 + s)
        if s < STEPS:
            dst[4 + s] = joint_ref[s - 1, 0]
            dst[5 + s] = joint_ref[s - 1, 1]
            value = mlat[4] * g
            if s > 1:
                value = value + center[3] * rest + west(plon[3] * rest) + east(mlon[3] * rest)
            if s > 2:
                value = value + plat[2] * behind
            behind = mlat[3] * rest if s > 1 else None
            rest = value
        done(s, dst)


def prepare_kernel(
    lon_hbm, lat_hbm, jac_hbm, field_ref, prec_ref, rows_ref, counts_ref, oprec_ref,
    coef_ref, prec_out, weight_ref, joint_ref, end_ref, jac_ref, lon, lat, x0, x1, sems,
):
    core = lax.axis_index("ens")
    lons = lon.shape[-1]
    levels = lon.shape[0]
    copies = [
        fetch(source, 0, 2 * HALF, target, sems.at[i])
        for i, (source, target) in enumerate(((lon_hbm, lon), (lat_hbm, lat)))
    ]
    for copy in copies:
        copy.start()
    jac_copy = pltpu.make_async_copy(jac_hbm.at[0], jac_ref, sems.at[2])
    jac_copy.start()
    level = lax.broadcasted_iota(jnp.int32, prec_out.shape, 0)
    prec = jnp.zeros(prec_out.shape, jnp.float32)
    for k in range(levels):
        prec = jnp.where(level == k, prec_ref[k], prec)
    prec_out[...] = prec
    slot = lax.broadcasted_iota(jnp.int32, weight_ref.shape, 0)
    mine = (rows_ref[...] % 16) // HALF == core
    weight_ref[...] = jnp.where((slot < counts_ref[...]) & mine, oprec_ref[...], 0.0)
    for copy in copies:
        copy.wait()

    def rows(at, sign):
        for r in range(12):
            coef_ref[1, r, :, 0:lons] = lon[:, at(r), :]
            wrap(coef_ref.at[1, r], lons)
            coef_ref[4, r, :, 0:lons] = sign * lat[:, at(r), :]
            wrap(coef_ref.at[4, r], lons)
            store_coefficients(coef_ref, r, coef_ref[1, r], coef_ref[4, r])

    @pl.when(core == 0)
    def _():
        rows(lambda r: r, 1.0)

    @pl.when(core == 1)
    def _():
        rows(lambda r: 15 - r, -1.0)

    x0[4:16] = field_ref[...]
    coefs = [Rows(None, coef_ref, i) for i in range(5)]

    def done(step, dst):
        if step == STEPS:
            end_ref[...] = dst[8:12]

    inner_steps(forward_step, (x0, x1), coefs, joint_ref, done)
    jac_copy.wait()


def store_coefficients(coef_ref, at, c, e):
    cc = c * c
    ee = e * e
    coef_ref[0, at] = 1.0 - cc - ee
    coef_ref[1, at] = 0.5 * (cc - c)
    coef_ref[2, at] = 0.5 * (cc + c)
    coef_ref[3, at] = 0.5 * (ee - e)
    coef_ref[4, at] = 0.5 * (ee + e)


def forward_kernel(
    field_ref, coef_ref, joint_ref, far_ref, halo_ref, jac, rows_hbm, val_ref, weight_ref,
    end_ref, force_ref, edge_ref, x0, x1, pk, wgt, rows, sem,
):
    core = lax.axis_index("ens")
    blocks, slots, lons = jac.shape
    rows_copy = pltpu.make_async_copy(rows_hbm, rows, sem)
    rows_copy.start()
    x0[3] = halo_ref[0]
    x0[4:6] = field_ref[0:2]
    store_coefficients(edge_ref, 1, halo_ref[4], halo_ref[5])
    lat = halo_ref[6]
    edge_ref[3, 0] = 0.5 * (lat * lat - lat)
    coefs = [Rows(edge_ref, coef_ref, i) for i in range(5)]
    outer_forward((x0, x1), coefs, joint_ref, halo_ref)
    field = (x0, x1)[STEPS % 2]
    end_ref[0:4] = field[4:8]
    end_ref[4:8] = far_ref[...]
    force_ref[...] = jnp.zeros(force_ref.shape, jnp.float32)

    rows_copy.wait()

    def place(j):
        r = rows[0, j]
        lat = r % 16
        row = jnp.clip(jnp.where(core == 0, lat, 15 - lat), 0, HALF - 1)
        return row, pl.ds(r // 16, 1)

    for j in range(blocks):
        row, lev = place(j)
        pk[pl.ds(j, 1), :] = end_ref[row, lev, :]
    lane = lax.broadcasted_iota(jnp.int32, (slots, blocks), 1)
    ev = jnp.zeros((slots, blocks), jnp.float32)
    for j in range(blocks):
        total = jnp.sum(jac[j] * pk[pl.ds(j, 1), 0:lons], axis=1, keepdims=True)
        ev = jnp.where(lane == j, total, ev)
    wgt[...] = weight_ref[...] * (ev - val_ref[...])
    for j in range(blocks):
        w = jnp.sum(jnp.where(lane == j, wgt[...], 0.0), axis=1, keepdims=True)
        pk[pl.ds(j, 1), 0:lons] = jnp.sum(jac[j] * w, axis=0, keepdims=True)
    wrap(pk, lons)
    for j in range(blocks):
        row, lev = place(j)
        force_ref[row, lev, :] = force_ref[row, lev, :] + pk[pl.ds(j, 1), :]


def with_next():
    return (lax.axis_index(TM) < lax.axis_size(TM) - 1).astype(jnp.float32)


def near_kernel(force_ref, end_ref, next_ref, prec_ref, coef_ref, adj_ref, flux_ref, x0, x1):
    prec = prec_ref[...] * with_next()
    for r in range(4):
        adj = force_ref[r] - prec * (next_ref[r] - end_ref[r])
        adj_ref[r] = adj
        x0[r] = adj
    center, plon, mlon, plat, mlat = (coef_ref.at[i] for i in range(5))
    flux_ref[0] = mlat[0] * x0[0]
    for s in range(1, STEPS):
        src, dst = (x0, x1) if s % 2 else (x1, x0)
        for r in range(4 - s):
            g = src[r]
            value = center[r] * g + west(plon[r] * g) + east(mlon[r] * g) + mlat[r + 1] * src[r + 1]
            dst[r] = value + plat[r - 1] * src[r - 1] if r else value
        flux_ref[s] = mlat[0] * dst[0]


def far_kernel(force_ref, end_ref, near_ref, far_ref, prec_ref, later_ref, adj_ref, inner_ref):
    prec = prec_ref[...] * with_next()
    for r in range(4):
        later_ref[r] = prec * (near_ref[r] - end_ref[r])
        later = prec * (far_ref[r] - end_ref[4 + r])
        later_ref[4 + r] = later
        adj = force_ref[4 + r] - later
        adj_ref[r] = adj
        inner_ref[3 - r] = adj


def adjoint_inner_kernel(near_ref, adj_ref, inner_ref, coef_ref, joint_ref, far_ref, total_ref, g0, g1):
    g0[4:8] = near_ref[...]
    g0[8:12] = adj_ref[...]
    g0[12:16] = inner_ref[...]
    coefs = [Rows(None, coef_ref, i) for i in range(5)]
    total_ref[0:4] = near_ref[...]
    total_ref[4:8] = adj_ref[...]

    def done(step, dst):
        if step == STEPS:
            far_ref[...] = dst[8:12]
        else:
            for j in range(4 + step, 12):
                total_ref[j - 4] = total_ref[j - 4] + dst[j]

    inner_steps(adjoint_step, (g0, g1), coefs, joint_ref, done)


def adjoint_kernel(
    adj_ref, outer_ref, edge_ref, coef_ref, joint_ref, far_ref, total_ref, forcing_ref, start_ref, g0, g1, sums
):
    core = lax.axis_index("ens")
    lons = forcing_ref.shape[-1]
    g0[4:6] = adj_ref[0:2]
    coefs = [Rows(edge_ref, coef_ref, i) for i in range(5)]
    sums[...] = total_ref[0:3]
    start_ref[4:8] = far_ref[...]

    def done(step, dst):
        if step == STEPS:
            start_ref[0:4] = dst[4:8]
        else:
            for j in range(4, 4 + step):
                sums[j - 4] = sums[j - 4] + dst[j]

    outer_adjoint((g0, g1), coefs, joint_ref, outer_ref, done)

    def store(at):
        for r in range(HALF):
            forcing_ref[:, at(r), :] = (sums if r < 3 else total_ref)[r, :, 0:lons]

    @pl.when(core == 0)
    def _():
        store(lambda r: r)

    @pl.when(core == 1)
    def _():
        store(lambda r: 7 - r)


def mismatch_kernel(start_ref, mismatch_ref, near_ref, far_ref, prec_ref, grad_ref):
    first_window = lax.axis_index(TM) == 0
    prec = prec_ref[...]
    for r in range(HALF):
        inc = (near_ref if r < 4 else far_ref)[r % 4]
        grad_ref[r] = start_ref[r] + jnp.where(first_window, prec * inc, mismatch_ref[r])


def product_kernel(pieces_ref, own_ref, other_ref, out_ref):
    core = lax.axis_index("ens")
    forcing = jnp.sum(pieces_ref[...], axis=0)
    lane = lax.broadcasted_iota(jnp.int32, (HALF, LANES), 1)
    members = own_ref.shape[0]
    first = pl.multiple_of(HALF * core, HALF)
    vec = jnp.zeros((HALF, LANES), jnp.float32)
    for m in range(2 * members):
        ref, at = (own_ref, m) if m < members else (other_ref, m - members)
        col = jnp.sum(ref[at, 0, pl.ds(first, HALF), :] * forcing, axis=1, keepdims=True)
        vec = jnp.where(lane == m, col, vec)
    vec = jnp.sum(vec, axis=0, keepdims=True)
    out_ref[...] = jnp.broadcast_to(vec[None], out_ref.shape)


def sum_kernel(sums_ref, out_ref):
    vec = jnp.sum(sums_ref[...], axis=0)
    out_ref[...] = jnp.broadcast_to(vec, out_ref.shape)


def final_kernel(sum_ref, other_sum_ref, own_ref, other_ref, own_grad_ref, other_grad_ref, out_ref, grad_ref):
    store_gradient(own_grad_ref, other_grad_ref, grad_ref)
    members = own_ref.shape[0]
    lane = lax.broadcasted_iota(jnp.int32, (HALF, LANES), 1)
    theirs = other_sum_ref[...]
    swapped = jnp.where(
        lane < members, pltpu.roll(theirs, LANES - members, 1), pltpu.roll(theirs, members, 1)
    )
    vec = (sum_ref[...] + swapped) * (-1.0 / (MEM - 1.0))
    coefs = [jnp.sum(jnp.where(lane == m, vec, 0.0), axis=1, keepdims=True) for m in range(2 * members)]
    for half in range(2):
        rows = pl.ds(HALF * half, HALF)
        total = coefs[0] * own_ref[0, 0, rows, :]
        for m in range(1, 2 * members):
            ref, at = (own_ref, m) if m < members else (other_ref, m - members)
            total = total + coefs[m] * ref[at, 0, rows, :]
        out_ref[0, rows, :] = total


def store_gradient(own_ref, other_ref, out_ref):
    core = lax.axis_index("ens")
    lons = out_ref.shape[-1]

    def store(north, south):
        for r in range(HALF):
            out_ref[0, :, r, :] = north[r, :, 0:lons]
            out_ref[0, :, 15 - r, :] = south[r, :, 0:lons]

    @pl.when(core == 0)
    def _():
        store(own_ref, other_ref)

    @pl.when(core == 1)
    def _():
        store(other_ref, own_ref)


VMEM = pl.BlockSpec(memory_space=pltpu.VMEM)
SMEM = pl.BlockSpec(memory_space=pltpu.SMEM)
HBM = pl.BlockSpec(memory_space=pltpu.HBM)


def buf(*shape):
    return pltpu.VMEM(shape, jnp.float32)


def in_hbm(value):
    return pltpu.with_memory_space_constraint(value, pltpu.HBM)


def call(kernel, ins, outs, scratch=(), limit=40):
    return pl.pallas_call(
        kernel,
        out_shape=[jax.ShapeDtypeStruct(s, jnp.float32) for s in outs],
        in_specs=ins,
        out_specs=[VMEM] * len(outs),
        scratch_shapes=list(scratch),
        compiler_params=pltpu.CompilerParams(vmem_limit_bytes=int(limit * 2**20)),
    )


def on_device(
    increment,
    wind_lon,
    wind_lat,
    model_precision,
    perturbations,
    obs_rows,
    obs_jacobian,
    obs_values,
    obs_precision,
    obs_counts,
):
    count_t = lax.axis_size(TM)
    count_l = lax.axis_size(LAT)
    levels, band_rows, lons = increment.shape[1:]
    wide = lons + (-lons % LANES)
    blocks, slots = obs_values.shape[1:]

    trade = []
    for i in range(count_l - 1):
        trade += [(2 * i + 1, 2 * i + 2), (2 * i + 2, 2 * i + 1)]
    band = LAT + ("ens",)
    partner = [(0, 1), (1, 0)]
    own = (HALF, levels, wide)
    quarter = (4, levels, wide)
    fields = (increment, wind_lon, wind_lat)
    piece = buf(levels, HALF, lons)
    whole = buf(levels, band_rows, lons)

    row = buf(4, levels, wide)
    (outgoing,) = call(
        edge_kernel,
        [HBM] * 3,
        [(7, levels, wide)],
        [piece, piece, piece, row, row, buf(5, 3, levels, wide), pltpu.SemaphoreType.DMA((3,))],
    )(*(in_hbm(field) for field in fields))
    halo = lax.ppermute(outgoing, band, trade)
    near_rows, far_rows, field = call(own_kernel, [VMEM], [quarter, quarter, (12, levels, wide)])(increment)
    earlier = [(i + 1, i) for i in range(count_t - 1)]
    next_near = lax.ppermute(near_rows, TM, earlier)
    next_far = lax.ppermute(far_rows, TM, earlier)
    working = buf(16, levels, wide)
    joint = (STEPS - 1, 2, levels, wide)
    coefs, prec, weight, joint_rows, far, jacobian = call(
        prepare_kernel,
        [HBM] * 3 + [VMEM, SMEM] + [VMEM] * 3,
        [(5, 12, levels, wide), (levels, wide), (slots, blocks), joint, quarter, (blocks, slots, lons)],
        [whole, whole, working, working, pltpu.SemaphoreType.DMA((3,))],
    )(in_hbm(wind_lon), in_hbm(wind_lat), in_hbm(obs_jacobian), field, model_precision, obs_rows, obs_counts, obs_precision[0].T)
    other_pert = lax.ppermute(perturbations, "ens", partner)

    end, force, edges = call(
        forward_kernel,
        [VMEM] * 6 + [HBM] + [VMEM] * 2,
        [own, own, (5, 2, levels, wide)],
        [
            working, working, buf(blocks, wide), buf(slots, blocks),
            pltpu.SMEM((1, blocks), jnp.int32), pltpu.SemaphoreType.DMA,
        ],
    )(field, coefs, joint_rows, far, halo, jacobian, in_hbm(obs_rows), obs_values[0].T, weight)
    near, outer = call(near_kernel, [VMEM] * 5, [quarter, quarter], [buf(*quarter), buf(*quarter)])(force, end, next_near, prec, coefs)
    outer = lax.ppermute(outer, band, trade)
    later, adj, inner = call(far_kernel, [VMEM] * 5, [own, quarter, quarter])(
        force, end, next_near, next_far, prec
    )
    inner = lax.ppermute(inner, "ens", partner)
    mismatch = lax.ppermute(later, TM, [(i, i + 1) for i in range(count_t - 1)])
    joint_rows, far, total = call(
        adjoint_inner_kernel, [VMEM] * 4, [joint, quarter, own], [working, working]
    )(near, adj, inner, coefs)
    forcing, start = call(
        adjoint_kernel,
        [VMEM] * 7,
        [(levels, HALF, lons), own],
        [working, working, buf(3, levels, wide)],
    )(near, outer, edges, coefs, joint_rows, far, total)
    pieces = lax.all_to_all(forcing, TM, 0, 0, tiled=True)

    (products,) = call(product_kernel, [VMEM] * 3, [(count_t * count_l, 1, LANES)])(
        pieces, perturbations, other_pert
    )
    start, mismatch, products = lax.optimization_barrier((start, mismatch, products))
    (own_grad,) = call(mismatch_kernel, [VMEM] * 5, [own])(start, mismatch, near_rows, far_rows, prec)
    other_grad = lax.ppermute(own_grad, "ens", partner)
    sums = lax.all_to_all(products, TM_LAT, 0, 0, tiled=True)
    (total,) = call(sum_kernel, [VMEM], [(HALF, LANES)])(sums)
    other_total = lax.ppermute(total, "ens", partner)
    forcing_step, grad_state = call(
        final_kernel, [VMEM] * 6, [(1, band_rows, lons), (1, levels, band_rows, lons)]
    )(total, other_total, perturbations, other_pert, own_grad, other_grad)
    return (grad_state, forcing_step)


def solution(mesh):
    torus = Mesh(
        mesh.devices.reshape(2, 4, 8, 2, mesh.shape["ens"]),
        ("tm_0", "tm_1", "lat_0", "lat_1", "ens"),
    )
    in_specs = (
        P(TM, None, LAT, None),
        P(TM, None, LAT, None),
        P(TM, None, LAT, None),
        P(),
        P("ens", TM, LAT, None),
        P(TM, LAT),
        P(TM, LAT, None, None),
        P(TM, LAT, None),
        P(TM, LAT, None),
        P(TM, LAT),
    )
    out_specs = (P(TM, None, LAT, None), P(TM, LAT, None))

    return jax.shard_map(on_device, mesh=torus, in_specs=in_specs, out_specs=out_specs, check_vma=False)
```

```python
import jax
import jax.numpy as jnp
from jax import lax
from jax.experimental import pallas as pl
from jax.experimental.pallas import tpu as pltpu
from jax.sharding import Mesh
from jax.sharding import PartitionSpec as P

MEM = 32
STEPS = 4
LANES = 128
HALF = 8
TM = ("tm_0", "tm_1")
LAT = ("lat_0", "lat_1")
TM_LAT = ("tm_0", "tm_1", "lat_0", "lat_1")


def east(value):
    return pltpu.roll(value, value.shape[-1] - 1, 1)


def west(value):
    return pltpu.roll(value, 1, 1)


def wrap(ref, lons):
    tail = lons % LANES
    half = (LANES - tail) // 2
    first = ref[:, 0:LANES]
    lane = lax.broadcasted_iota(jnp.int32, first.shape, 1)
    last = jnp.where(lane < tail, ref[:, lons - tail :], 0.0)
    ref[:, lons - tail :] = jnp.where(
        lane < tail, last, jnp.where(lane < tail + half, pltpu.roll(first, tail, 1), pltpu.roll(last, LANES - tail, 1))
    )


def edge_kernel(inc_hbm, lon_hbm, lat_hbm, out_ref, inc, lon, lat, x0, x1, coef, sems):
    core = lax.axis_index("ens")
    lons = inc.shape[-1]

    def rows(at, sign):
        first = 0 if at(0) == 0 else HALF
        copies = []
        for part, start in enumerate((first, HALF - first)):
            for i, (source, target) in enumerate(((inc_hbm, inc), (lon_hbm, lon), (lat_hbm, lat))):
                where = (0, slice(None), pl.ds(start, HALF), slice(None))
                copies.append(pltpu.make_async_copy(source.at[where], target.at[where], sems.at[3 * part + i]))
        for copy in copies:
            copy.start()
        copies[0].wait()
        for r in range(4):
            x0[r, :, 0:lons] = inc[0, :, at(r), :]
            wrap(x0.at[r], lons)
        copies[1].wait()
        copies[2].wait()
        for r in range(3):
            coef[1, r, :, 0:lons] = lon[0, :, at(r), :]
            wrap(coef.at[1, r], lons)
            coef[4, r, :, 0:lons] = sign * lat[0, :, at(r), :]
            wrap(coef.at[4, r], lons)
            c, e = coef[1, r], coef[4, r]
            if r == 0:
                out_ref[4] = c
                out_ref[5] = -e
            if r == 1:
                out_ref[6] = -e
            store_coefficients(coef, r, c, e)
        out_ref[0] = x0[0]
        for s in range(1, STEPS):
            src, dst = (x0, x1) if s % 2 else (x1, x0)
            for r in range(4 - s):
                f = src[r]
                value = coef[0, r] * f + coef[1, r] * east(f) + coef[2, r] * west(f) + coef[3, r] * src[r + 1]
                dst[r] = value + coef[4, r] * src[r - 1] if r else value
            out_ref[s] = dst[0]
        for copy in copies[3:]:
            copy.wait()

    @pl.when(core == 0)
    def _():
        rows(lambda r: r, 1.0)

    @pl.when(core == 1)
    def _():
        rows(lambda r: 15 - r, -1.0)


def own_kernel(inc_ref, near_ref, far_ref, field_ref):
    core = lax.axis_index("ens")
    lons = inc_ref.shape[-1]

    def rows(at):
        for r in range(12):
            field_ref[r, :, 0:lons] = inc_ref[0, :, at(r), :]
            wrap(field_ref.at[r], lons)
            if r < HALF:
                (near_ref if r < 4 else far_ref)[r % 4] = field_ref[r]

    @pl.when(core == 0)
    def _():
        rows(lambda r: r)

    @pl.when(core == 1)
    def _():
        rows(lambda r: 15 - r)


class Rows:
    def __init__(self, halo_ref, own_ref, at):
        self.halo, self.own, self.at = halo_ref, own_ref, at

    def __getitem__(self, j):
        return self.halo[self.at, j - 2] if j < 4 else self.own[self.at, j - 4]


def forward_step(src, dst, coefs, first, last):
    center, plon, mlon, plat, mlat = coefs
    for j in range(first, last):
        f = src[j]
        dst[j] = center[j] * f + plon[j] * east(f) + mlon[j] * west(f) + plat[j] * src[j + 1] + mlat[j] * src[j - 1]


def adjoint_step(src, dst, coefs, first, last):
    center, plon, mlon, plat, mlat = coefs
    for j in range(first, last):
        g = src[j]
        dst[j] = (
            center[j] * g
            + west(plon[j] * g)
            + east(mlon[j] * g)
            + plat[j - 1] * src[j - 1]
            + mlat[j + 1] * src[j + 1]
        )


def inner_steps(step_of, bufs, coefs, joint_ref, done):
    for s in range(1, STEPS + 1):
        src, dst = bufs[(s - 1) % 2], bufs[s % 2]
        step_of(src, dst, coefs, 4 + s, 16 - s)
        if s < STEPS:
            joint_ref[s - 1, 0] = dst[4 + s]
            joint_ref[s - 1, 1] = dst[5 + s]
        done(s, dst)


def outer_forward(bufs, coefs, joint_ref, halo_ref):
    center, plon, mlon, plat, mlat = coefs
    behind = rest = None
    for s in range(1, STEPS + 1):
        src, dst = bufs[(s - 1) % 2], bufs[s % 2]
        forward_step(src, dst, coefs, 4, 4 + s)
        if s < STEPS:
            dst[4 + s] = joint_ref[s - 1, 0]
            dst[5 + s] = joint_ref[s - 1, 1]
            value = plat[3] * src[4]
            if s > 1:
                value = value + center[3] * rest + plon[3] * east(rest) + mlon[3] * west(rest)
            if s > 2:
                value = value + mlat[3] * behind
            behind = plat[2] * rest if s > 1 else None
            rest = value
            dst[3] = halo_ref[s] + rest


def outer_adjoint(bufs, coefs, joint_ref, flux_ref, done):
    center, plon, mlon, plat, mlat = coefs
    behind = rest = None
    for s in range(1, STEPS + 1):
        src, dst = bufs[(s - 1) % 2], bufs[s % 2]
        g = src[4]
        flux = flux_ref[s - 1] if s == 1 else flux_ref[s - 1] + plat[3] * rest
        dst[4] = center[4] * g + west(plon[4] * g) + east(mlon[4] * g) + flux + mlat[5] * src[5]
        adjoint_step(src, dst, coefs, 5, 4 + s)
        if s < STEPS:
            dst[4 + s] = joint_ref[s - 1, 0]
            dst[5 + s] = joint_ref[s - 1, 1]
            value = mlat[4] * g
            if s > 1:
                value = value + center[3] * rest + west(plon[3] * rest) + east(mlon[3] * rest)
            if s > 2:
                value = value + plat[2] * behind
            behind = mlat[3] * rest if s > 1 else None
            rest = value
        done(s, dst)


def prepare_kernel(
    lon_ref, lat_ref, jac_hbm, field_ref, prec_ref, rows_ref, counts_ref, oprec_ref,
    coef_ref, prec_out, weight_ref, joint_ref, end_ref, jac_ref, x0, x1, sem,
):
    core = lax.axis_index("ens")
    lons = lon_ref.shape[-1]
    levels = prec_out.shape[0]
    jac_copy = pltpu.make_async_copy(jac_hbm.at[0], jac_ref, sem)
    jac_copy.start()
    level = lax.broadcasted_iota(jnp.int32, prec_out.shape, 0)
    prec = jnp.zeros(prec_out.shape, jnp.float32)
    for k in range(levels):
        prec = jnp.where(level == k, prec_ref[k], prec)
    prec_out[...] = prec
    slot = lax.broadcasted_iota(jnp.int32, weight_ref.shape, 0)
    mine = (rows_ref[...] % 16) // HALF == core
    weight_ref[...] = jnp.where((slot < counts_ref[...]) & mine, oprec_ref[...], 0.0)

    def rows(at, sign):
        for r in range(12):
            coef_ref[1, r, :, 0:lons] = lon_ref[0, :, at(r), :]
            wrap(coef_ref.at[1, r], lons)
            coef_ref[4, r, :, 0:lons] = sign * lat_ref[0, :, at(r), :]
            wrap(coef_ref.at[4, r], lons)
            store_coefficients(coef_ref, r, coef_ref[1, r], coef_ref[4, r])

    @pl.when(core == 0)
    def _():
        rows(lambda r: r, 1.0)

    @pl.when(core == 1)
    def _():
        rows(lambda r: 15 - r, -1.0)

    x0[4:16] = field_ref[...]
    coefs = [Rows(None, coef_ref, i) for i in range(5)]

    def done(step, dst):
        if step == STEPS:
            end_ref[...] = dst[8:12]

    inner_steps(forward_step, (x0, x1), coefs, joint_ref, done)
    jac_copy.wait()


def store_coefficients(coef_ref, at, c, e):
    cc = c * c
    ee = e * e
    coef_ref[0, at] = 1.0 - cc - ee
    coef_ref[1, at] = 0.5 * (cc - c)
    coef_ref[2, at] = 0.5 * (cc + c)
    coef_ref[3, at] = 0.5 * (ee - e)
    coef_ref[4, at] = 0.5 * (ee + e)


def forward_kernel(
    field_ref, coef_ref, joint_ref, far_ref, halo_ref, jac, rows_hbm, val_ref, weight_ref,
    end_ref, force_ref, edge_ref, x0, x1, pk, wgt, rows, sem,
):
    core = lax.axis_index("ens")
    blocks, slots, lons = jac.shape
    rows_copy = pltpu.make_async_copy(rows_hbm, rows, sem)
    rows_copy.start()
    x0[3] = halo_ref[0]
    x0[4:6] = field_ref[0:2]
    store_coefficients(edge_ref, 1, halo_ref[4], halo_ref[5])
    lat = halo_ref[6]
    edge_ref[3, 0] = 0.5 * (lat * lat - lat)
    coefs = [Rows(edge_ref, coef_ref, i) for i in range(5)]
    outer_forward((x0, x1), coefs, joint_ref, halo_ref)
    field = (x0, x1)[STEPS % 2]
    end_ref[0:4] = field[4:8]
    end_ref[4:8] = far_ref[...]
    force_ref[...] = jnp.zeros(force_ref.shape, jnp.float32)

    rows_copy.wait()

    def place(j):
        r = rows[0, j]
        lat = r % 16
        row = jnp.clip(jnp.where(core == 0, lat, 15 - lat), 0, HALF - 1)
        return row, pl.ds(r // 16, 1)

    for j in range(blocks):
        row, lev = place(j)
        pk[pl.ds(j, 1), :] = end_ref[row, lev, :]
    lane = lax.broadcasted_iota(jnp.int32, (slots, blocks), 1)
    ev = jnp.zeros((slots, blocks), jnp.float32)
    for j in range(blocks):
        total = jnp.sum(jac[j] * pk[pl.ds(j, 1), 0:lons], axis=1, keepdims=True)
        ev = jnp.where(lane == j, total, ev)
    wgt[...] = weight_ref[...] * (ev - val_ref[...])
    for j in range(blocks):
        w = jnp.sum(jnp.where(lane == j, wgt[...], 0.0), axis=1, keepdims=True)
        pk[pl.ds(j, 1), 0:lons] = jnp.sum(jac[j] * w, axis=0, keepdims=True)
    wrap(pk, lons)
    for j in range(blocks):
        row, lev = place(j)
        force_ref[row, lev, :] = force_ref[row, lev, :] + pk[pl.ds(j, 1), :]


def with_next():
    return (lax.axis_index(TM) < lax.axis_size(TM) - 1).astype(jnp.float32)


def near_kernel(force_ref, end_ref, next_ref, prec_ref, coef_ref, adj_ref, flux_ref, x0, x1):
    prec = prec_ref[...] * with_next()
    for r in range(4):
        adj = force_ref[r] - prec * (next_ref[r] - end_ref[r])
        adj_ref[r] = adj
        x0[r] = adj
    center, plon, mlon, plat, mlat = (coef_ref.at[i] for i in range(5))
    flux_ref[0] = mlat[0] * x0[0]
    for s in range(1, STEPS):
        src, dst = (x0, x1) if s % 2 else (x1, x0)
        for r in range(4 - s):
            g = src[r]
            value = center[r] * g + west(plon[r] * g) + east(mlon[r] * g) + mlat[r + 1] * src[r + 1]
            dst[r] = value + plat[r - 1] * src[r - 1] if r else value
        flux_ref[s] = mlat[0] * dst[0]


def far_kernel(force_ref, end_ref, near_ref, far_ref, prec_ref, later_ref, adj_ref, inner_ref):
    prec = prec_ref[...] * with_next()
    for r in range(4):
        later_ref[r] = prec * (near_ref[r] - end_ref[r])
        later = prec * (far_ref[r] - end_ref[4 + r])
        later_ref[4 + r] = later
        adj = force_ref[4 + r] - later
        adj_ref[r] = adj
        inner_ref[3 - r] = adj


def adjoint_inner_kernel(near_ref, adj_ref, inner_ref, coef_ref, joint_ref, far_ref, total_ref, g0, g1):
    g0[4:8] = near_ref[...]
    g0[8:12] = adj_ref[...]
    g0[12:16] = inner_ref[...]
    coefs = [Rows(None, coef_ref, i) for i in range(5)]
    total_ref[0:4] = near_ref[...]
    total_ref[4:8] = adj_ref[...]

    def done(step, dst):
        if step == STEPS:
            far_ref[...] = dst[8:12]
        else:
            for j in range(4 + step, 12):
                total_ref[j - 4] = total_ref[j - 4] + dst[j]

    inner_steps(adjoint_step, (g0, g1), coefs, joint_ref, done)


def adjoint_kernel(
    adj_ref, outer_ref, edge_ref, coef_ref, joint_ref, far_ref, total_ref, forcing_ref, start_ref, g0, g1, sums
):
    core = lax.axis_index("ens")
    lons = forcing_ref.shape[-1]
    g0[4:6] = adj_ref[0:2]
    coefs = [Rows(edge_ref, coef_ref, i) for i in range(5)]
    sums[...] = total_ref[0:3]
    start_ref[4:8] = far_ref[...]

    def done(step, dst):
        if step == STEPS:
            start_ref[0:4] = dst[4:8]
        else:
            for j in range(4, 4 + step):
                sums[j - 4] = sums[j - 4] + dst[j]

    outer_adjoint((g0, g1), coefs, joint_ref, outer_ref, done)

    def store(at):
        for r in range(HALF):
            forcing_ref[:, at(r), :] = (sums if r < 3 else total_ref)[r, :, 0:lons]

    @pl.when(core == 0)
    def _():
        store(lambda r: r)

    @pl.when(core == 1)
    def _():
        store(lambda r: 7 - r)


def mismatch_kernel(start_ref, mismatch_ref, near_ref, far_ref, prec_ref, grad_ref):
    first_window = lax.axis_index(TM) == 0
    prec = prec_ref[...]
    for r in range(HALF):
        inc = (near_ref if r < 4 else far_ref)[r % 4]
        grad_ref[r] = start_ref[r] + jnp.where(first_window, prec * inc, mismatch_ref[r])


def product_kernel(pieces_ref, own_ref, other_ref, out_ref):
    core = lax.axis_index("ens")
    forcing = jnp.sum(pieces_ref[...], axis=0)
    lane = lax.broadcasted_iota(jnp.int32, (HALF, LANES), 1)
    members = own_ref.shape[0]
    first = pl.multiple_of(HALF * core, HALF)
    vec = jnp.zeros((HALF, LANES), jnp.float32)
    for m in range(2 * members):
        ref, at = (own_ref, m) if m < members else (other_ref, m - members)
        col = jnp.sum(ref[at, 0, pl.ds(first, HALF), :] * forcing, axis=1, keepdims=True)
        vec = jnp.where(lane == m, col, vec)
    vec = jnp.sum(vec, axis=0, keepdims=True)
    out_ref[...] = jnp.broadcast_to(vec[None], out_ref.shape)


def sum_kernel(sums_ref, out_ref):
    vec = jnp.sum(sums_ref[...], axis=0)
    out_ref[...] = jnp.broadcast_to(vec, out_ref.shape)


def step_kernel(sum_ref, other_sum_ref, own_ref, other_ref, out_ref):
    members = own_ref.shape[0]
    lane = lax.broadcasted_iota(jnp.int32, (HALF, LANES), 1)
    theirs = other_sum_ref[...]
    swapped = jnp.where(
        lane < members, pltpu.roll(theirs, LANES - members, 1), pltpu.roll(theirs, members, 1)
    )
    vec = (sum_ref[...] + swapped) * (-1.0 / (MEM - 1.0))
    coefs = [jnp.sum(jnp.where(lane == m, vec, 0.0), axis=1, keepdims=True) for m in range(2 * members)]
    for half in range(2):
        rows = pl.ds(HALF * half, HALF)
        total = coefs[0] * own_ref[0, 0, rows, :]
        for m in range(1, 2 * members):
            ref, at = (own_ref, m) if m < members else (other_ref, m - members)
            total = total + coefs[m] * ref[at, 0, rows, :]
        out_ref[0, rows, :] = total


def gradient_kernel(own_ref, other_ref, out_ref):
    core = lax.axis_index("ens")
    lons = out_ref.shape[-1]

    def store(north, south):
        for r in range(HALF):
            out_ref[0, :, r, :] = north[r, :, 0:lons]
            out_ref[0, :, 15 - r, :] = south[r, :, 0:lons]

    @pl.when(core == 0)
    def _():
        store(own_ref, other_ref)

    @pl.when(core == 1)
    def _():
        store(other_ref, own_ref)


VMEM = pl.BlockSpec(memory_space=pltpu.VMEM)
SMEM = pl.BlockSpec(memory_space=pltpu.SMEM)
HBM = pl.BlockSpec(memory_space=pltpu.HBM)


def buf(*shape):
    return pltpu.VMEM(shape, jnp.float32)


def in_hbm(value):
    return pltpu.with_memory_space_constraint(value, pltpu.HBM)


def call(kernel, ins, outs, scratch=(), limit=40):
    return pl.pallas_call(
        kernel,
        out_shape=[jax.ShapeDtypeStruct(s, jnp.float32) for s in outs],
        in_specs=ins,
        out_specs=[VMEM] * len(outs),
        scratch_shapes=list(scratch),
        compiler_params=pltpu.CompilerParams(vmem_limit_bytes=int(limit * 2**20)),
    )


def on_device(
    increment,
    wind_lon,
    wind_lat,
    model_precision,
    perturbations,
    obs_rows,
    obs_jacobian,
    obs_values,
    obs_precision,
    obs_counts,
):
    count_t = lax.axis_size(TM)
    count_l = lax.axis_size(LAT)
    levels, band_rows, lons = increment.shape[1:]
    wide = lons + (-lons % LANES)
    blocks, slots = obs_values.shape[1:]

    trade = []
    for i in range(count_l - 1):
        trade += [(2 * i + 1, 2 * i + 2), (2 * i + 2, 2 * i + 1)]
    band = LAT + ("ens",)
    partner = [(0, 1), (1, 0)]
    own = (HALF, levels, wide)
    quarter = (4, levels, wide)
    fields = (increment, wind_lon, wind_lat)

    row = buf(4, levels, wide)
    whole = (1, levels, band_rows, lons)
    outgoing, inc_band, lon_band, lat_band = call(
        edge_kernel,
        [HBM] * 3,
        [(7, levels, wide), whole, whole, whole],
        [row, row, buf(5, 3, levels, wide), pltpu.SemaphoreType.DMA((6,))],
    )(*(in_hbm(field) for field in fields))
    halo = lax.ppermute(outgoing, band, trade)
    near_rows, far_rows, field = call(own_kernel, [VMEM], [quarter, quarter, (12, levels, wide)])(inc_band)
    earlier = [(i + 1, i) for i in range(count_t - 1)]
    next_near = lax.ppermute(near_rows, TM, earlier)
    next_far = lax.ppermute(far_rows, TM, earlier)
    working = buf(16, levels, wide)
    joint = (STEPS - 1, 2, levels, wide)
    coefs, prec, weight, joint_rows, far, jacobian = call(
        prepare_kernel,
        [VMEM, VMEM, HBM, VMEM, SMEM] + [VMEM] * 3,
        [(5, 12, levels, wide), (levels, wide), (slots, blocks), joint, quarter, (blocks, slots, lons)],
        [working, working, pltpu.SemaphoreType.DMA],
    )(lon_band, lat_band, in_hbm(obs_jacobian), field, model_precision, obs_rows, obs_counts, obs_precision[0].T)
    other_pert = lax.ppermute(perturbations, "ens", partner)

    end, force, edges = call(
        forward_kernel,
        [VMEM] * 6 + [HBM] + [VMEM] * 2,
        [own, own, (5, 2, levels, wide)],
        [
            working, working, buf(blocks, wide), buf(slots, blocks),
            pltpu.SMEM((1, blocks), jnp.int32), pltpu.SemaphoreType.DMA,
        ],
    )(field, coefs, joint_rows, far, halo, jacobian, in_hbm(obs_rows), obs_values[0].T, weight)
    near, outer = call(near_kernel, [VMEM] * 5, [quarter, quarter], [buf(*quarter), buf(*quarter)])(force, end, next_near, prec, coefs)
    outer = lax.ppermute(outer, band, trade)
    later, adj, inner = call(far_kernel, [VMEM] * 5, [own, quarter, quarter])(
        force, end, next_near, next_far, prec
    )
    inner = lax.ppermute(inner, "ens", partner)
    mismatch = lax.ppermute(later, TM, [(i, i + 1) for i in range(count_t - 1)])
    joint_rows, far, total = call(
        adjoint_inner_kernel, [VMEM] * 4, [joint, quarter, own], [working, working]
    )(near, adj, inner, coefs)
    forcing, start = call(
        adjoint_kernel,
        [VMEM] * 7,
        [(levels, HALF, lons), own],
        [working, working, buf(3, levels, wide)],
    )(near, outer, edges, coefs, joint_rows, far, total)
    pieces = lax.all_to_all(forcing, TM, 0, 0, tiled=True)

    (products,) = call(product_kernel, [VMEM] * 3, [(count_t * count_l, 1, LANES)])(
        pieces, perturbations, other_pert
    )
    start, mismatch, products = lax.optimization_barrier((start, mismatch, products))
    (own_grad,) = call(mismatch_kernel, [VMEM] * 5, [own])(start, mismatch, near_rows, far_rows, prec)
    other_grad = lax.ppermute(own_grad, "ens", partner)
    sums = lax.all_to_all(products, TM_LAT, 0, 0, tiled=True)
    (total,) = call(sum_kernel, [VMEM], [(HALF, LANES)])(sums)
    other_total = lax.ppermute(total, "ens", partner)
    (grad_state,) = call(gradient_kernel, [VMEM] * 2, [whole])(own_grad, other_grad)
    (forcing_step,) = call(step_kernel, [VMEM] * 4, [(1, band_rows, lons)])(
        total, other_total, perturbations, other_pert
    )
    return (grad_state, forcing_step)


def solution(mesh):
    torus = Mesh(
        mesh.devices.reshape(2, 4, 8, 2, mesh.shape["ens"]),
        ("tm_0", "tm_1", "lat_0", "lat_1", "ens"),
    )
    in_specs = (
        P(TM, None, LAT, None),
        P(TM, None, LAT, None),
        P(TM, None, LAT, None),
        P(),
        P("ens", TM, LAT, None),
        P(TM, LAT),
        P(TM, LAT, None, None),
        P(TM, LAT, None),
        P(TM, LAT, None),
        P(TM, LAT),
    )
    out_specs = (P(TM, None, LAT, None), P(TM, LAT, None))

    return jax.shard_map(on_device, mesh=torus, in_specs=in_specs, out_specs=out_specs, check_vma=False)
```

```python
import jax
import jax.numpy as jnp
from jax import lax
from jax.experimental import pallas as pl
from jax.experimental.pallas import tpu as pltpu
from jax.sharding import Mesh
from jax.sharding import PartitionSpec as P

MEM = 32
STEPS = 4
LANES = 128
HALF = 8
TM = ("tm_0", "tm_1")
LAT = ("lat_0", "lat_1")
LAT_TM = ("lat_0", "lat_1", "tm_0", "tm_1")


def east(value):
    return pltpu.roll(value, value.shape[-1] - 1, 1)


def west(value):
    return pltpu.roll(value, 1, 1)


def wrap(ref, lons):
    tail = lons % LANES
    half = (LANES - tail) // 2
    first = ref[:, 0:LANES]
    lane = lax.broadcasted_iota(jnp.int32, first.shape, 1)
    last = jnp.where(lane < tail, ref[:, lons - tail :], 0.0)
    ref[:, lons - tail :] = jnp.where(
        lane < tail, last, jnp.where(lane < tail + half, pltpu.roll(first, tail, 1), pltpu.roll(last, LANES - tail, 1))
    )


def pack(ref, count, lons, out_ref):
    full, tail = lons // LANES, lons % LANES
    share = LANES // tail
    lane = lax.broadcasted_iota(jnp.int32, (HALF, LANES), 1)
    for r in range(count):
        for i in range(full):
            out_ref[full * r + i] = ref[r, :, LANES * i : LANES * (i + 1)]
    for first in range(0, count, share):
        ends = ref[first, :, full * LANES :]
        for q in range(1, min(share, count - first)):
            end = pltpu.roll(ref[first + q, :, full * LANES :], tail * q, 1)
            ends = jnp.where(lane < tail * q, ends, end)
        out_ref[full * count + first // share] = ends


def unpack(in_ref, count, lons, ref):
    full, tail = lons // LANES, lons % LANES
    share = LANES // tail
    for r in range(count):
        for i in range(full):
            ref[r, :, LANES * i : LANES * (i + 1)] = in_ref[full * r + i]
        ends = in_ref[full * count + r // share]
        q = r % share
        ref[r, :, full * LANES :] = pltpu.roll(ends, LANES - tail * q, 1) if q else ends
        wrap(ref.at[r], lons)


def tiles(count, levels, lons):
    share = LANES // (lons % LANES)
    return (lons // LANES * count + -(-count // share), levels, LANES)


def edge_kernel(inc_hbm, lon_hbm, lat_hbm, packed_ref, inc, lon, lat, out_ref, x0, x1, coef, sems):
    core = lax.axis_index("ens")
    lons = inc.shape[-1]

    def rows(at, sign):
        first = 0 if at(0) == 0 else HALF
        copies = []
        for part, start in enumerate((first, HALF - first)):
            for i, (source, target) in enumerate(((inc_hbm, inc), (lon_hbm, lon), (lat_hbm, lat))):
                where = (0, slice(None), pl.ds(start, HALF), slice(None))
                copies.append(pltpu.make_async_copy(source.at[where], target.at[where], sems.at[3 * part + i]))
        for copy in copies:
            copy.start()
        copies[0].wait()
        for r in range(4):
            x0[r, :, 0:lons] = inc[0, :, at(r), :]
            wrap(x0.at[r], lons)
        copies[1].wait()
        copies[2].wait()
        for r in range(3):
            coef[1, r, :, 0:lons] = lon[0, :, at(r), :]
            wrap(coef.at[1, r], lons)
            coef[4, r, :, 0:lons] = sign * lat[0, :, at(r), :]
            wrap(coef.at[4, r], lons)
            c, e = coef[1, r], coef[4, r]
            if r == 0:
                out_ref[4] = c
                out_ref[5] = -e
            if r == 1:
                out_ref[6] = -e
            store_coefficients(coef, r, c, e)
        out_ref[0] = x0[0]
        for s in range(1, STEPS):
            src, dst = (x0, x1) if s % 2 else (x1, x0)
            for r in range(4 - s):
                f = src[r]
                value = coef[0, r] * f + coef[1, r] * east(f) + coef[2, r] * west(f) + coef[3, r] * src[r + 1]
                dst[r] = value + coef[4, r] * src[r - 1] if r else value
            out_ref[s] = dst[0]
        pack(out_ref, 7, lons, packed_ref)
        for copy in copies[3:]:
            copy.wait()

    @pl.when(core == 0)
    def _():
        rows(lambda r: r, 1.0)

    @pl.when(core == 1)
    def _():
        rows(lambda r: 15 - r, -1.0)


def own_kernel(inc_ref, near_ref, far_ref, near_packed, far_packed, field_ref):
    core = lax.axis_index("ens")
    lons = inc_ref.shape[-1]

    def rows(at):
        for r in range(12):
            field_ref[r, :, 0:lons] = inc_ref[0, :, at(r), :]
            wrap(field_ref.at[r], lons)
            if r < HALF:
                (near_ref if r < 4 else far_ref)[r % 4] = field_ref[r]

    @pl.when(core == 0)
    def _():
        rows(lambda r: r)

    @pl.when(core == 1)
    def _():
        rows(lambda r: 15 - r)

    pack(near_ref, 4, lons, near_packed)
    pack(far_ref, 4, lons, far_packed)


class Rows:
    def __init__(self, halo_ref, own_ref, at):
        self.halo, self.own, self.at = halo_ref, own_ref, at

    def __getitem__(self, j):
        return self.halo[self.at, j - 2] if j < 4 else self.own[self.at, j - 4]


def forward_step(src, dst, coefs, first, last):
    center, plon, mlon, plat, mlat = coefs
    for j in range(first, last):
        f = src[j]
        dst[j] = center[j] * f + plon[j] * east(f) + mlon[j] * west(f) + plat[j] * src[j + 1] + mlat[j] * src[j - 1]


def adjoint_step(src, dst, coefs, first, last):
    center, plon, mlon, plat, mlat = coefs
    for j in range(first, last):
        g = src[j]
        dst[j] = (
            center[j] * g
            + west(plon[j] * g)
            + east(mlon[j] * g)
            + plat[j - 1] * src[j - 1]
            + mlat[j + 1] * src[j + 1]
        )


def inner_steps(step_of, bufs, coefs, joint_ref, done):
    for s in range(1, STEPS + 1):
        src, dst = bufs[(s - 1) % 2], bufs[s % 2]
        step_of(src, dst, coefs, 4 + s, 16 - s)
        if s < STEPS:
            joint_ref[s - 1, 0] = dst[4 + s]
            joint_ref[s - 1, 1] = dst[5 + s]
        done(s, dst)


def outer_forward(bufs, coefs, joint_ref, halo_ref):
    center, plon, mlon, plat, mlat = coefs
    behind = rest = None
    for s in range(1, STEPS + 1):
        src, dst = bufs[(s - 1) % 2], bufs[s % 2]
        forward_step(src, dst, coefs, 4, 4 + s)
        if s < STEPS:
            dst[4 + s] = joint_ref[s - 1, 0]
            dst[5 + s] = joint_ref[s - 1, 1]
            value = plat[3] * src[4]
            if s > 1:
                value = value + center[3] * rest + plon[3] * east(rest) + mlon[3] * west(rest)
            if s > 2:
                value = value + mlat[3] * behind
            behind = plat[2] * rest if s > 1 else None
            rest = value
            dst[3] = halo_ref[s] + rest


def outer_adjoint(bufs, coefs, joint_ref, flux_ref, done):
    center, plon, mlon, plat, mlat = coefs
    behind = rest = None
    for s in range(1, STEPS + 1):
        src, dst = bufs[(s - 1) % 2], bufs[s % 2]
        g = src[4]
        flux = flux_ref[s - 1] if s == 1 else flux_ref[s - 1] + plat[3] * rest
        dst[4] = center[4] * g + west(plon[4] * g) + east(mlon[4] * g) + flux + mlat[5] * src[5]
        adjoint_step(src, dst, coefs, 5, 4 + s)
        if s < STEPS:
            dst[4 + s] = joint_ref[s - 1, 0]
            dst[5 + s] = joint_ref[s - 1, 1]
            value = mlat[4] * g
            if s > 1:
                value = value + center[3] * rest + west(plon[3] * rest) + east(mlon[3] * rest)
            if s > 2:
                value = value + plat[2] * behind
            behind = mlat[3] * rest if s > 1 else None
            rest = value
        done(s, dst)


def prepare_kernel(
    lon_ref, lat_ref, jac_hbm, field_ref, prec_ref, rows_ref, counts_ref, oprec_ref,
    coef_ref, prec_out, weight_ref, joint_ref, end_ref, jac_ref, x0, x1, sem,
):
    core = lax.axis_index("ens")
    lons = lon_ref.shape[-1]
    levels = prec_out.shape[0]
    jac_copy = pltpu.make_async_copy(jac_hbm.at[0], jac_ref, sem)
    jac_copy.start()
    level = lax.broadcasted_iota(jnp.int32, prec_out.shape, 0)
    prec = jnp.zeros(prec_out.shape, jnp.float32)
    for k in range(levels):
        prec = jnp.where(level == k, prec_ref[k], prec)
    prec_out[...] = prec
    slot = lax.broadcasted_iota(jnp.int32, weight_ref.shape, 0)
    mine = (rows_ref[...] % 16) // HALF == core
    weight_ref[...] = jnp.where((slot < counts_ref[...]) & mine, oprec_ref[...], 0.0)

    def rows(at, sign):
        for r in range(12):
            coef_ref[1, r, :, 0:lons] = lon_ref[0, :, at(r), :]
            wrap(coef_ref.at[1, r], lons)
            coef_ref[4, r, :, 0:lons] = sign * lat_ref[0, :, at(r), :]
            wrap(coef_ref.at[4, r], lons)
            store_coefficients(coef_ref, r, coef_ref[1, r], coef_ref[4, r])

    @pl.when(core == 0)
    def _():
        rows(lambda r: r, 1.0)

    @pl.when(core == 1)
    def _():
        rows(lambda r: 15 - r, -1.0)

    x0[4:16] = field_ref[...]
    coefs = [Rows(None, coef_ref, i) for i in range(5)]

    def done(step, dst):
        if step == STEPS:
            end_ref[...] = dst[8:12]

    inner_steps(forward_step, (x0, x1), coefs, joint_ref, done)
    jac_copy.wait()


def store_coefficients(coef_ref, at, c, e):
    cc = c * c
    ee = e * e
    coef_ref[0, at] = 1.0 - cc - ee
    coef_ref[1, at] = 0.5 * (cc - c)
    coef_ref[2, at] = 0.5 * (cc + c)
    coef_ref[3, at] = 0.5 * (ee - e)
    coef_ref[4, at] = 0.5 * (ee + e)


def forward_kernel(
    field_ref, coef_ref, joint_ref, far_ref, packed_ref, jac, rows_hbm, val_ref, weight_ref,
    end_ref, force_ref, edge_ref, halo_ref, x0, x1, pk, wgt, rows, sem,
):
    core = lax.axis_index("ens")
    blocks, slots, lons = jac.shape
    rows_copy = pltpu.make_async_copy(rows_hbm, rows, sem)
    rows_copy.start()
    unpack(packed_ref, 7, lons, halo_ref)
    x0[3] = halo_ref[0]
    x0[4:6] = field_ref[0:2]
    store_coefficients(edge_ref, 1, halo_ref[4], halo_ref[5])
    lat = halo_ref[6]
    edge_ref[3, 0] = 0.5 * (lat * lat - lat)
    coefs = [Rows(edge_ref, coef_ref, i) for i in range(5)]
    outer_forward((x0, x1), coefs, joint_ref, halo_ref)
    field = (x0, x1)[STEPS % 2]
    end_ref[0:4] = field[4:8]
    end_ref[4:8] = far_ref[...]
    force_ref[...] = jnp.zeros(force_ref.shape, jnp.float32)

    rows_copy.wait()

    def place(j):
        r = rows[0, j]
        lat = r % 16
        row = jnp.clip(jnp.where(core == 0, lat, 15 - lat), 0, HALF - 1)
        return row, pl.ds(r // 16, 1)

    for j in range(blocks):
        row, lev = place(j)
        pk[pl.ds(j, 1), :] = end_ref[row, lev, :]
    lane = lax.broadcasted_iota(jnp.int32, (slots, blocks), 1)
    ev = jnp.zeros((slots, blocks), jnp.float32)
    for j in range(blocks):
        total = jnp.sum(jac[j] * pk[pl.ds(j, 1), 0:lons], axis=1, keepdims=True)
        ev = jnp.where(lane == j, total, ev)
    wgt[...] = weight_ref[...] * (ev - val_ref[...])
    for j in range(blocks):
        w = jnp.sum(jnp.where(lane == j, wgt[...], 0.0), axis=1, keepdims=True)
        pk[pl.ds(j, 1), 0:lons] = jnp.sum(jac[j] * w, axis=0, keepdims=True)
    wrap(pk, lons)
    for j in range(blocks):
        row, lev = place(j)
        force_ref[row, lev, :] = force_ref[row, lev, :] + pk[pl.ds(j, 1), :]


def with_next():
    return (lax.axis_index(TM) < lax.axis_size(TM) - 1).astype(jnp.float32)


def near_kernel(force_ref, end_ref, packed_ref, prec_ref, coef_ref, adj_ref, flux_packed, later_ref, next_ref, flux_ref, x0, x1):
    lons = 1440
    unpack(packed_ref, 4, lons, next_ref)
    prec = prec_ref[...] * with_next()
    for r in range(4):
        later = prec * (next_ref[r] - end_ref[r])
        later_ref[r] = later
        adj = force_ref[r] - later
        adj_ref[r] = adj
        x0[r] = adj
    center, plon, mlon, plat, mlat = (coef_ref.at[i] for i in range(5))
    flux_ref[0] = mlat[0] * x0[0]
    for s in range(1, STEPS):
        src, dst = (x0, x1) if s % 2 else (x1, x0)
        for r in range(4 - s):
            g = src[r]
            value = center[r] * g + west(plon[r] * g) + east(mlon[r] * g) + mlat[r + 1] * src[r + 1]
            dst[r] = value + plat[r - 1] * src[r - 1] if r else value
        flux_ref[s] = mlat[0] * dst[0]
    pack(flux_ref, 4, lons, flux_packed)


def far_kernel(force_ref, end_ref, near_ref, packed_ref, prec_ref, later_ref, adj_ref, inner_ref, next_ref):
    unpack(packed_ref, 4, 1440, next_ref)
    prec = prec_ref[...] * with_next()
    for r in range(4):
        later_ref[r] = near_ref[r]
        later = prec * (next_ref[r] - end_ref[4 + r])
        later_ref[4 + r] = later
        adj = force_ref[4 + r] - later
        adj_ref[r] = adj
        inner_ref[3 - r] = adj


def adjoint_inner_kernel(near_ref, adj_ref, inner_ref, coef_ref, joint_ref, far_ref, total_ref, g0, g1):
    g0[4:8] = near_ref[...]
    g0[8:12] = adj_ref[...]
    g0[12:16] = inner_ref[...]
    coefs = [Rows(None, coef_ref, i) for i in range(5)]
    total_ref[0:4] = near_ref[...]
    total_ref[4:8] = adj_ref[...]

    def done(step, dst):
        if step == STEPS:
            far_ref[...] = dst[8:12]
        else:
            for j in range(4 + step, 12):
                total_ref[j - 4] = total_ref[j - 4] + dst[j]

    inner_steps(adjoint_step, (g0, g1), coefs, joint_ref, done)


def adjoint_kernel(
    adj_ref, packed_ref, edge_ref, coef_ref, joint_ref, far_ref, total_ref, forcing_ref, start_ref, outer_ref, g0, g1, sums
):
    core = lax.axis_index("ens")
    lons = forcing_ref.shape[-1]
    unpack(packed_ref, 4, lons, outer_ref)
    g0[4:6] = adj_ref[0:2]
    coefs = [Rows(edge_ref, coef_ref, i) for i in range(5)]
    sums[...] = total_ref[0:3]
    start_ref[4:8] = far_ref[...]

    def done(step, dst):
        if step == STEPS:
            start_ref[0:4] = dst[4:8]
        else:
            for j in range(4, 4 + step):
                sums[j - 4] = sums[j - 4] + dst[j]

    outer_adjoint((g0, g1), coefs, joint_ref, outer_ref, done)

    def store(at):
        for r in range(HALF):
            forcing_ref[:, at(r), :] = (sums if r < 3 else total_ref)[r, :, 0:lons]

    @pl.when(core == 0)
    def _():
        store(lambda r: r)

    @pl.when(core == 1)
    def _():
        store(lambda r: 7 - r)


def mismatch_kernel(start_ref, mismatch_ref, near_ref, far_ref, prec_ref, grad_ref):
    first_window = lax.axis_index(TM) == 0
    prec = prec_ref[...]
    for r in range(HALF):
        inc = (near_ref if r < 4 else far_ref)[r % 4]
        grad_ref[r] = start_ref[r] + jnp.where(first_window, prec * inc, mismatch_ref[r])


def product_kernel(pieces_ref, own_ref, other_ref, out_ref):
    core = lax.axis_index("ens")
    forcing = jnp.sum(pieces_ref[...], axis=0)
    lane = lax.broadcasted_iota(jnp.int32, (HALF, LANES), 1)
    members = own_ref.shape[0]
    first = pl.multiple_of(HALF * core, HALF)
    vec = jnp.zeros((HALF, LANES), jnp.float32)
    for m in range(2 * members):
        ref, at = (own_ref, m) if m < members else (other_ref, m - members)
        col = jnp.sum(ref[at, 0, pl.ds(first, HALF), :] * forcing, axis=1, keepdims=True)
        vec = jnp.where(lane == m, col, vec)
    vec = jnp.sum(vec, axis=0, keepdims=True)
    out_ref[...] = jnp.broadcast_to(vec[None], out_ref.shape)


def sum_kernel(sums_ref, out_ref):
    vec = jnp.sum(sums_ref[...], axis=0)
    out_ref[...] = jnp.broadcast_to(vec, out_ref.shape)


def step_kernel(sum_ref, other_sum_ref, own_ref, other_ref, out_ref):
    members = own_ref.shape[0]
    lane = lax.broadcasted_iota(jnp.int32, (HALF, LANES), 1)
    theirs = other_sum_ref[...]
    swapped = jnp.where(
        lane < members, pltpu.roll(theirs, LANES - members, 1), pltpu.roll(theirs, members, 1)
    )
    vec = (sum_ref[...] + swapped) * (-1.0 / (MEM - 1.0))
    coefs = [jnp.sum(jnp.where(lane == m, vec, 0.0), axis=1, keepdims=True) for m in range(2 * members)]
    for half in range(2):
        rows = pl.ds(HALF * half, HALF)
        total = coefs[0] * own_ref[0, 0, rows, :]
        for m in range(1, 2 * members):
            ref, at = (own_ref, m) if m < members else (other_ref, m - members)
            total = total + coefs[m] * ref[at, 0, rows, :]
        out_ref[0, rows, :] = total


def gradient_kernel(own_ref, other_ref, out_ref):
    core = lax.axis_index("ens")
    lons = out_ref.shape[-1]

    def store(north, south):
        for r in range(HALF):
            out_ref[0, :, r, :] = north[r, :, 0:lons]
            out_ref[0, :, 15 - r, :] = south[r, :, 0:lons]

    @pl.when(core == 0)
    def _():
        store(own_ref, other_ref)

    @pl.when(core == 1)
    def _():
        store(other_ref, own_ref)


VMEM = pl.BlockSpec(memory_space=pltpu.VMEM)
SMEM = pl.BlockSpec(memory_space=pltpu.SMEM)
HBM = pl.BlockSpec(memory_space=pltpu.HBM)


def buf(*shape):
    return pltpu.VMEM(shape, jnp.float32)


def in_hbm(value):
    return pltpu.with_memory_space_constraint(value, pltpu.HBM)


def call(kernel, ins, outs, scratch=(), limit=40):
    return pl.pallas_call(
        kernel,
        out_shape=[jax.ShapeDtypeStruct(s, jnp.float32) for s in outs],
        in_specs=ins,
        out_specs=[VMEM] * len(outs),
        scratch_shapes=list(scratch),
        compiler_params=pltpu.CompilerParams(vmem_limit_bytes=int(limit * 2**20)),
    )


def on_device(
    increment,
    wind_lon,
    wind_lat,
    model_precision,
    perturbations,
    obs_rows,
    obs_jacobian,
    obs_values,
    obs_precision,
    obs_counts,
):
    count_t = lax.axis_size(TM)
    count_l = lax.axis_size(LAT)
    levels, band_rows, lons = increment.shape[1:]
    wide = lons + (-lons % LANES)
    blocks, slots = obs_values.shape[1:]

    trade = []
    for i in range(count_l - 1):
        trade += [(2 * i + 1, 2 * i + 2), (2 * i + 2, 2 * i + 1)]
    band = LAT + ("ens",)
    partner = [(0, 1), (1, 0)]
    own = (HALF, levels, wide)
    quarter = (4, levels, wide)
    fields = (increment, wind_lon, wind_lat)

    row = buf(4, levels, wide)
    whole = (1, levels, band_rows, lons)
    outgoing, inc_band, lon_band, lat_band = call(
        edge_kernel,
        [HBM] * 3,
        [tiles(7, levels, lons), whole, whole, whole],
        [buf(7, levels, wide), row, row, buf(5, 3, levels, wide), pltpu.SemaphoreType.DMA((6,))],
    )(*(in_hbm(field) for field in fields))
    halo = lax.ppermute(outgoing, band, trade)
    packed = tiles(4, levels, lons)
    near_rows, far_rows, near_packed, far_packed, field = call(
        own_kernel, [VMEM], [quarter, quarter, packed, packed, (12, levels, wide)]
    )(inc_band)
    earlier = [(i + 1, i) for i in range(count_t - 1)]
    next_near = lax.ppermute(near_packed, TM, earlier)
    working = buf(16, levels, wide)
    joint = (STEPS - 1, 2, levels, wide)
    coefs, prec, weight, joint_rows, far, jacobian = call(
        prepare_kernel,
        [VMEM, VMEM, HBM, VMEM, SMEM] + [VMEM] * 3,
        [(5, 12, levels, wide), (levels, wide), (slots, blocks), joint, quarter, (blocks, slots, lons)],
        [working, working, pltpu.SemaphoreType.DMA],
    )(lon_band, lat_band, in_hbm(obs_jacobian), field, model_precision, obs_rows, obs_counts, obs_precision[0].T)
    other_pert = lax.ppermute(perturbations, "ens", partner)

    far_packed, far = lax.optimization_barrier((far_packed, far))
    next_far = lax.ppermute(far_packed, TM, earlier)
    end, force, edges = call(
        forward_kernel,
        [VMEM] * 6 + [HBM] + [VMEM] * 2,
        [own, own, (5, 2, levels, wide)],
        [
            buf(7, levels, wide), working, working, buf(blocks, wide), buf(slots, blocks),
            pltpu.SMEM((1, blocks), jnp.int32), pltpu.SemaphoreType.DMA,
        ],
    )(field, coefs, joint_rows, far, halo, jacobian, in_hbm(obs_rows), obs_values[0].T, weight)
    near, outer, later = call(near_kernel, [VMEM] * 5, [quarter, packed, quarter], [buf(*quarter)] * 4)(force, end, next_near, prec, coefs)
    outer = lax.ppermute(outer, band, trade)
    later, adj, inner = call(far_kernel, [VMEM] * 5, [own, quarter, quarter], [buf(*quarter)])(
        force, end, later, next_far, prec
    )
    inner = lax.ppermute(inner, "ens", partner)
    mismatch = lax.ppermute(later, TM, [(i, i + 1) for i in range(count_t - 1)])
    joint_rows, far, total = call(
        adjoint_inner_kernel, [VMEM] * 4, [joint, quarter, own], [working, working]
    )(near, adj, inner, coefs)
    forcing, start = call(
        adjoint_kernel,
        [VMEM] * 7,
        [(levels, HALF, lons), own],
        [buf(*quarter), working, working, buf(3, levels, wide)],
    )(near, outer, edges, coefs, joint_rows, far, total)
    pieces = lax.all_to_all(forcing, TM, 0, 0, tiled=True)

    (products,) = call(product_kernel, [VMEM] * 3, [(count_t * count_l, 1, LANES)])(
        pieces, perturbations, other_pert
    )
    start, mismatch, products = lax.optimization_barrier((start, mismatch, products))
    (own_grad,) = call(mismatch_kernel, [VMEM] * 5, [own])(start, mismatch, near_rows, far_rows, prec)
    other_grad = lax.ppermute(own_grad, "ens", partner)
    sums = lax.all_to_all(products, LAT_TM, 0, 0, tiled=True)
    (total,) = call(sum_kernel, [VMEM], [(HALF, LANES)])(sums)
    other_total = lax.ppermute(total, "ens", partner)
    (grad_state,) = call(gradient_kernel, [VMEM] * 2, [whole])(own_grad, other_grad)
    (forcing_step,) = call(step_kernel, [VMEM] * 4, [(1, band_rows, lons)])(
        total, other_total, perturbations, other_pert
    )
    return (grad_state, forcing_step)


def solution(mesh):
    torus = Mesh(
        mesh.devices.reshape(2, 4, 8, 2, mesh.shape["ens"]),
        ("tm_0", "tm_1", "lat_0", "lat_1", "ens"),
    )
    in_specs = (
        P(TM, None, LAT, None),
        P(TM, None, LAT, None),
        P(TM, None, LAT, None),
        P(),
        P("ens", TM, LAT, None),
        P(TM, LAT),
        P(TM, LAT, None, None),
        P(TM, LAT, None),
        P(TM, LAT, None),
        P(TM, LAT),
    )
    out_specs = (P(TM, None, LAT, None), P(TM, LAT, None))

    return jax.shard_map(on_device, mesh=torus, in_specs=in_specs, out_specs=out_specs, check_vma=False)
```
